32 devices in a mesh: data: 32 (over z, y, x, core).
Axes of the slice: x: 2, y: 2, z: 4, core: 2. Of those that a mesh axis runs over, the one named last changes fastest.
Arguments:
- x_in: bfloat16 [32, 384, 768], P('data')
- grad_y: bfloat16 [32, 384, 768], P('data')
- gain_one: float32 [3, 768], replicated
- gain_two: float32 [3, 768], replicated
- w_qkv: bfloat16 [3, 768, 2304], replicated
- w_out: bfloat16 [3, 768, 768], replicated
- w_up: bfloat16 [3, 768, 3072], replicated
- w_down: bfloat16 [3, 3072, 768], replicated
Outputs:
- output 1: bfloat16 [32, 384, 768], P('data')
- output 2: float32 [3, 768], replicated
- output 3: float32 [3, 768], replicated
- output 4: float32 [3, 768, 2304], replicated
- output 5: float32 [3, 768, 768], replicated
- output 6: float32 [3, 768, 3072], replicated
- output 7: float32 [3, 3072, 768], replicated
All inputs are finite; a program needn't handle non-finite values.
Results may differ from the reference program's by a relative error of at most 0.02.
Values are sent between devices in bfloat16 or wider.
A program may use at most 1 GiB of HBM per device.

```python
import jax
import jax.numpy as jnp
from jax import lax

D = 768
FF = 3072
HEADS = 12
LAYERS = 3
SEQ = 384
BATCH = 32
GROUP = 32
HEAD_DIM = D // HEADS
NORM_EPS = 1e-6


def setup_inputs(seed: int = 0) -> dict:
    root_key = jax.random.key(seed)
    sub_keys = jax.random.split(root_key, 8)
    x_in = jax.random.normal(sub_keys[0], (BATCH, SEQ, D), jnp.float32)
    grad_y = jax.random.normal(sub_keys[1], (BATCH, SEQ, D), jnp.float32)
    gain_one = 1.0 + 0.3 * jax.random.normal(sub_keys[2], (LAYERS, D), jnp.float32)
    gain_two = 1.0 + 0.3 * jax.random.normal(sub_keys[3], (LAYERS, D), jnp.float32)
    w_qkv = jax.random.normal(sub_keys[4], (LAYERS, D, 3 * D), jnp.float32) * D ** -0.5
    w_out = jax.random.normal(sub_keys[5], (LAYERS, D, D), jnp.float32) * D ** -0.5
    w_up = jax.random.normal(sub_keys[6], (LAYERS, D, FF), jnp.float32) * D ** -0.5
    w_down = jax.random.normal(sub_keys[7], (LAYERS, FF, D), jnp.float32) * FF ** -0.5
    return {'x_in': x_in.astype(jnp.bfloat16), 'grad_y': grad_y.astype(jnp.bfloat16), 'gain_one': gain_one, 'gain_two': gain_two, 'w_qkv': w_qkv.astype(jnp.bfloat16), 'w_out': w_out.astype(jnp.bfloat16), 'w_up': w_up.astype(jnp.bfloat16), 'w_down': w_down.astype(jnp.bfloat16)}


def rms_gain(rows_f, gain_vec):
    return rows_f * lax.rsqrt(jnp.mean(rows_f * rows_f, axis=-1, keepdims=True) + NORM_EPS) * gain_vec


def gelu_tanh(pre_act):
    return jax.nn.gelu(pre_act, approximate=True)


def mat_lo(lhs_mat, rhs_mat):
    return jnp.dot(lhs_mat, rhs_mat, preferred_element_type=jnp.float32).astype(jnp.bfloat16)


def mat_nt(lhs_mat, rhs_mat):
    return lax.dot_general(lhs_mat, rhs_mat, (((1,), (1,)), ((), ())), preferred_element_type=jnp.float32).astype(jnp.bfloat16)


def mat_tn(lhs_mat, rhs_mat):
    return lax.dot_general(lhs_mat, rhs_mat, (((0,), (0,)), ((), ())), preferred_element_type=jnp.float32)


def head_mix(einsum_spec, lhs_arr, rhs_arr):
    return jnp.einsum(einsum_spec, lhs_arr.astype(jnp.float32), rhs_arr.astype(jnp.float32))


def seq_forward(seq_rows, gain_a, gain_b, w_qkv, w_out, w_up):
    norm_a, norm_a_back = jax.vjp(rms_gain, seq_rows.astype(jnp.float32), gain_a)
    u_one = norm_a.astype(jnp.bfloat16)
    qkv_lo = mat_lo(u_one, w_qkv)
    q_all = qkv_lo[:, :D].reshape(SEQ, HEADS, HEAD_DIM)
    k_all = qkv_lo[:, D:2 * D].reshape(SEQ, HEADS, HEAD_DIM)
    v_all = qkv_lo[:, 2 * D:].reshape(SEQ, HEADS, HEAD_DIM)
    scores = head_mix('qhe,khe->hqk', q_all, k_all) * HEAD_DIM ** -0.5
    causal = jnp.arange(SEQ)[:, None] >= jnp.arange(SEQ)[None, :]
    prob_full = jax.nn.softmax(jnp.where(causal, scores, -1e30), axis=-1)
    prob_lo = prob_full.astype(jnp.bfloat16)
    attn_out = head_mix('hqk,khe->qhe', prob_lo, v_all).astype(jnp.bfloat16).reshape(SEQ, D)
    hidden = seq_rows + mat_lo(attn_out, w_out)
    norm_b, norm_b_back = jax.vjp(rms_gain, hidden.astype(jnp.float32), gain_b)
    u_two = norm_b.astype(jnp.bfloat16)
    pre_lo = mat_lo(u_two, w_up)
    act_f, gelu_back = jax.vjp(gelu_tanh, pre_lo.astype(jnp.float32))
    act_lo = act_f.astype(jnp.bfloat16)
    saved_vals = (norm_a_back, u_one, q_all, k_all, v_all, prob_full, prob_lo, attn_out, norm_b_back, u_two, gelu_back, act_lo)
    return hidden, act_lo, saved_vals


def seq_backward(grad_blk, saved_vals, w_qkv, w_out, w_up, w_down):
    (norm_a_back, u_one, q_all, k_all, v_all, prob_full, prob_lo, attn_out, norm_b_back, u_two, gelu_back, act_lo) = saved_vals
    grad_down_w = mat_tn(act_lo, grad_blk)
    grad_act = mat_nt(grad_blk, w_down)
    (grad_pre_f,) = gelu_back(grad_act.astype(jnp.float32))
    grad_pre = grad_pre_f.astype(jnp.bfloat16)
    grad_up_w = mat_tn(u_two, grad_pre)
    grad_u_two = mat_nt(grad_pre, w_up)
    grad_h_norm, grad_gain_b = norm_b_back(grad_u_two.astype(jnp.float32))
    grad_hidden = (grad_blk.astype(jnp.float32) + grad_h_norm).astype(jnp.bfloat16)
    grad_out_w = mat_tn(attn_out, grad_hidden)
    grad_attn = mat_nt(grad_hidden, w_out).reshape(SEQ, HEADS, HEAD_DIM)
    grad_probs = head_mix('qhe,khe->hqk', grad_attn, v_all)
    grad_scores = (prob_full * (grad_probs - jnp.sum(prob_full * grad_probs, axis=-1, keepdims=True)) * HEAD_DIM ** -0.5).astype(jnp.bfloat16)
    grad_v = head_mix('hqk,qhe->khe', prob_lo, grad_attn).astype(jnp.bfloat16)
    grad_q = head_mix('hqk,khe->qhe', grad_scores, k_all).astype(jnp.bfloat16)
    grad_k = head_mix('hqk,qhe->khe', grad_scores, q_all).astype(jnp.bfloat16)
    grad_qkv = jnp.concatenate([grad_q.reshape(SEQ, D), grad_k.reshape(SEQ, D), grad_v.reshape(SEQ, D)], axis=-1)
    grad_qkv_w = mat_tn(u_one, grad_qkv)
    grad_u_one = mat_nt(grad_qkv, w_qkv)
    grad_x_norm, grad_gain_a = norm_a_back(grad_u_one.astype(jnp.float32))
    grad_x_blk = (grad_hidden.astype(jnp.float32) + grad_x_norm).astype(jnp.bfloat16)
    return grad_x_blk, (grad_gain_a, grad_gain_b, grad_qkv_w, grad_out_w, grad_up_w, grad_down_w)


def reference(x_in, grad_y, gain_one, gain_two, w_qkv, w_out, w_up, w_down):
    def one_seq(grad_acc, seq_pair):
        seq_rows, seq_grad = seq_pair
        hidden_x = seq_rows
        saved_all = []
        for layer_idx in range(LAYERS):
            hidden, act_lo, saved_vals = seq_forward(hidden_x, gain_one[layer_idx], gain_two[layer_idx], w_qkv[layer_idx], w_out[layer_idx], w_up[layer_idx])
            saved_all.append(saved_vals)
            if layer_idx + 1 < LAYERS:
                hidden_x = hidden + mat_lo(act_lo, w_down[layer_idx])
        grad_cur = seq_grad
        grads_rev = []
        for layer_idx in reversed(range(LAYERS)):
            grad_cur, layer_grads = seq_backward(grad_cur, saved_all[layer_idx], w_qkv[layer_idx], w_out[layer_idx], w_up[layer_idx], w_down[layer_idx])
            grads_rev.append(layer_grads)
        grads_fwd = grads_rev[::-1]
        new_acc = tuple(grad_acc[grad_idx] + jnp.stack([layer_set[grad_idx] for layer_set in grads_fwd]) for grad_idx in range(6))
        return new_acc, grad_cur

    init_acc = (jnp.zeros((LAYERS, D), jnp.float32), jnp.zeros((LAYERS, D), jnp.float32), jnp.zeros((LAYERS, D, 3 * D), jnp.float32), jnp.zeros((LAYERS, D, D), jnp.float32), jnp.zeros((LAYERS, D, FF), jnp.float32), jnp.zeros((LAYERS, FF, D), jnp.float32))
    grad_sums, grad_x = lax.scan(one_seq, init_acc, (x_in, grad_y))
    return (grad_x, grad_sums[0] / GROUP, grad_sums[1] / GROUP, grad_sums[2] / GROUP, grad_sums[3] / GROUP, grad_sums[4] / GROUP, grad_sums[5] / GROUP)
```

```python
import functools

import jax
import jax.numpy as jnp
from jax import lax
from jax.experimental import pallas as pl
from jax.experimental.pallas import tpu as pltpu
from jax.sharding import PartitionSpec as P

NORM_EPS = 1e-6
HEAD_DIM = 64
WIDTH = 768
TILES = 12
SUB = 16
RING = 16
HOP = 2
MESH_ID = pl.DeviceIdType.MESH


def rms_gain(rows_f, gain_vec):
    return rows_f * lax.rsqrt(jnp.mean(rows_f * rows_f, axis=-1, keepdims=True) + NORM_EPS) * gain_vec


def gelu_tanh(pre_act):
    return jax.nn.gelu(pre_act, approximate=True)


def mix_lo(einsum_spec, lhs_arr, rhs_arr):
    return jnp.einsum(einsum_spec, lhs_arr, rhs_arr, preferred_element_type=jnp.float32).astype(jnp.bfloat16)


def mix_f32(einsum_spec, lhs_arr, rhs_arr):
    return jnp.einsum(einsum_spec, lhs_arr, rhs_arr, preferred_element_type=jnp.float32)


def block_forward(x_blk, gain_a, gain_b, w_qkv, w_out, w_up):
    n_batch, seq_len, width = x_blk.shape
    head_shape = (n_batch, seq_len, width // HEAD_DIM, HEAD_DIM)
    norm_a, norm_a_back = jax.vjp(rms_gain, x_blk.astype(jnp.float32), gain_a)
    u_one = norm_a.astype(jnp.bfloat16)
    qkv_lo = mix_lo('bsd,de->bse', u_one, w_qkv)
    q_all = qkv_lo[:, :, :width].reshape(head_shape)
    k_all = qkv_lo[:, :, width:2 * width].reshape(head_shape)
    v_all = qkv_lo[:, :, 2 * width:].reshape(head_shape)
    scores = mix_f32('bqhe,bkhe->bhqk', q_all, k_all) * HEAD_DIM ** -0.5
    causal = jnp.arange(seq_len)[:, None] >= jnp.arange(seq_len)[None, :]
    prob_full = jax.nn.softmax(jnp.where(causal, scores, -1e30), axis=-1)
    prob_lo = prob_full.astype(jnp.bfloat16)
    attn_out = mix_lo('bhqk,bkhe->bqhe', prob_lo, v_all).reshape(n_batch, seq_len, width)
    hidden = x_blk + mix_lo('bsd,de->bse', attn_out, w_out)
    norm_b, norm_b_back = jax.vjp(rms_gain, hidden.astype(jnp.float32), gain_b)
    u_two = norm_b.astype(jnp.bfloat16)
    pre_lo = mix_lo('bsd,df->bsf', u_two, w_up)
    act_f, gelu_back = jax.vjp(gelu_tanh, pre_lo.astype(jnp.float32))
    act_lo = act_f.astype(jnp.bfloat16)
    saved_vals = (norm_a_back, u_one, q_all, k_all, v_all, prob_full, prob_lo, attn_out, norm_b_back, u_two, gelu_back, act_lo)
    return hidden, act_lo, saved_vals


def block_backward(grad_blk, saved_vals, w_qkv, w_out, w_up, w_down):
    (norm_a_back, u_one, q_all, k_all, v_all, prob_full, prob_lo, attn_out, norm_b_back, u_two, gelu_back, act_lo) = saved_vals
    n_batch, seq_len, width = grad_blk.shape
    head_shape = (n_batch, seq_len, width // HEAD_DIM, HEAD_DIM)
    grad_act = mix_lo('bsd,fd->bsf', grad_blk, w_down)
    (grad_pre_f,) = gelu_back(grad_act.astype(jnp.float32))
    grad_pre = grad_pre_f.astype(jnp.bfloat16)
    grad_u_two = mix_lo('bsf,df->bsd', grad_pre, w_up)
    grad_h_norm, grad_gain_b = norm_b_back(grad_u_two.astype(jnp.float32))
    grad_hidden = (grad_blk.astype(jnp.float32) + grad_h_norm).astype(jnp.bfloat16)
    grad_attn = mix_lo('bse,de->bsd', grad_hidden, w_out).reshape(head_shape)
    grad_probs = mix_f32('bqhe,bkhe->bhqk', grad_attn, v_all)
    grad_scores = (prob_full * (grad_probs - jnp.sum(prob_full * grad_probs, axis=-1, keepdims=True)) * HEAD_DIM ** -0.5).astype(jnp.bfloat16)
    grad_v = mix_lo('bhqk,bqhe->bkhe', prob_lo, grad_attn)
    grad_q = mix_lo('bhqk,bkhe->bqhe', grad_scores, k_all)
    grad_k = mix_lo('bhqk,bqhe->bkhe', grad_scores, q_all)
    flat_shape = (n_batch, seq_len, width)
    grad_qkv = jnp.concatenate([grad_q.reshape(flat_shape), grad_k.reshape(flat_shape), grad_v.reshape(flat_shape)], axis=-1)
    grad_u_one = mix_lo('bse,de->bsd', grad_qkv, w_qkv)
    grad_x_norm, grad_gain_a = norm_a_back(grad_u_one.astype(jnp.float32))
    grad_x_blk = (grad_hidden.astype(jnp.float32) + grad_x_norm).astype(jnp.bfloat16)
    factors = (u_one, grad_qkv, attn_out, grad_hidden, u_two, grad_pre, act_lo, grad_blk)
    return grad_x_blk, grad_gain_a, grad_gain_b, factors


def layer_tiles(factors):
    u_one, grad_qkv, attn_out, grad_hidden, u_two, grad_pre, act_lo, grad_blk = factors
    tiles = []
    for lhs, rhs in ((u_one, grad_qkv), (attn_out, grad_hidden), (u_two, grad_pre), (act_lo, grad_blk)):
        tiles += [(lhs, left, rhs, right) for left in range(0, lhs.shape[1], WIDTH) for right in range(0, rhs.shape[1], WIDTH)]
    return tiles


def reduce_kernel(n_tile, n_dev, *refs):
    n_factor = 8 * (-(-n_tile // TILES))
    reduce_body(n_tile, n_dev, refs[:n_factor], *refs[n_factor:])


def reduce_body(n_tile, n_dev, f_refs, g_ref, fa, fb, part, ra, acc, rzb, rza, rb, fin,
                  fl_a, fl_b, fs_a, fs_b, fr_a, fr_b,
                  ra_s, ra_r, z_s, zb_r, za_r, b_s, b_r, bag_s, bag_r, loc, bc_r, up_s, dn_s, aag_s, aag_r, p1_s, p1_r, p2_s, p2_r):
    toks = f_refs[0].shape[0]
    half = WIDTH // 2
    n_slot = fa.shape[0]
    tiles = [tile for lo in range(0, len(f_refs), 8) for tile in layer_tiles(f_refs[lo:lo + 8])][:n_tile]
    per_tile = half // (8 * SUB)
    n_unit = n_tile * per_tile
    me = lax.axis_index('data')
    core, my_x, my_y, my_z = me % 2, (me // 2) % 2, (me // 4) % 2, me // 8
    top_z = n_dev // 8 - 1
    x_dev, y_dev, pair_dev = me + 2 - 4 * my_x, me + 4 - 8 * my_y, me + 1 - 2 * core
    up_dev, dn_dev = me + 8, me - 8

    barrier = pltpu.get_barrier_semaphore()
    for dev in (x_dev, y_dev, pair_dev):
        pl.semaphore_signal(barrier, inc=1, device_id=(dev,), device_id_type=MESH_ID)

    @pl.when(my_z < top_z)
    def _():
        pl.semaphore_signal(barrier, inc=1, device_id=(up_dev,), device_id_type=MESH_ID)

    @pl.when(my_z > 0)
    def _():
        pl.semaphore_signal(barrier, inc=1, device_id=(dn_dev,), device_id_type=MESH_ID)

    pl.semaphore_wait(barrier, 3 + jnp.where(my_z < top_z, 1, 0) + jnp.where(my_z > 0, 1, 0))

    def remote(src, dst, send_sem, recv_sem, dev):
        return pltpu.make_async_remote_copy(src_ref=src, dst_ref=dst, send_sem=send_sem, recv_sem=recv_sem, device_id=(dev,), device_id_type=MESH_ID)

    def factor_copies(slot, source):
        lhs, left, rhs, right = source
        mine = pl.ds(pl.multiple_of(left + core * half, 128), half)
        other = pl.ds(pl.multiple_of(left + (1 - core) * half, 128), half)
        lo, hi = pl.ds(0, toks), pl.ds(toks, toks)
        cols = pl.ds(right, WIDTH)
        return (
            pltpu.make_async_copy(lhs.at[:, mine], fa.at[slot, lo], fl_a.at[slot]),
            pltpu.make_async_copy(rhs.at[:, cols], fb.at[slot, lo], fl_b.at[slot]),
            remote(lhs.at[:, other], fa.at[slot, hi], fs_a.at[slot], fr_a.at[slot], pair_dev),
            remote(rhs.at[:, cols], fb.at[slot, hi], fs_b.at[slot], fr_b.at[slot], pair_dev),
        )

    for tile in range(2):
        for copy in factor_copies(tile, tiles[tile]):
            copy.start()

    def stream_stages(s):
        my_a, my_b = (my_x, my_y) if s == 0 else (my_y, my_x)
        a_dev, b_dev = (x_dev, y_dev) if s == 0 else (y_dev, x_dev)

        def root_of(u):
            return (u + 2 * s) % (top_z + 1)

        def part_rows(u, side):
            return pl.ds(pl.multiple_of((u % per_tile) * (8 * SUB) + s * (4 * SUB) + side * (2 * SUB), 8), 2 * SUB)

        def part_at(u, side):
            return part.at[(u // per_tile) % 2, part_rows(u, side)]

        def out_at(u, which, side, b_side=None):
            base = (u // per_tile) * WIDTH + which * half + (u % per_tile) * (8 * SUB) + s * (4 * SUB) + side * (2 * SUB)
            if b_side is None:
                return g_ref.at[pl.ds(pl.multiple_of(base, 8), 2 * SUB)]
            return g_ref.at[pl.ds(pl.multiple_of(base + b_side * SUB, 8), SUB)]

        def a_copy(u):
            k = u % RING
            return remote(part_at(u, 1 - my_a), ra.at[s, k], ra_s.at[s, k], ra_r.at[s, k], a_dev)

        def up_copy(u):
            k = u % RING
            return remote(acc.at[s, k], rzb.at[s, k], z_s.at[s, k], zb_r.at[s, k], up_dev)

        def dn_copy(u):
            k = u % RING
            return remote(acc.at[s, k], rza.at[s, k], z_s.at[s, k], za_r.at[s, k], dn_dev)

        def b_rows(side):
            return pl.ds(pl.multiple_of(side * SUB, 8), SUB)

        def b_copy(u):
            k = u % RING
            return remote(acc.at[s, k, b_rows(1 - my_b)], rb.at[s, k], b_s.at[s, k], b_r.at[s, k], b_dev)

        def bag_copy(u, b_side):
            k = u % RING
            return remote(fin.at[s, k], out_at(u, core, my_a, b_side), bag_s.at[s, k], bag_r.at[s, k], b_dev)

        def loc_copy(u):
            k = u % RING
            return pltpu.make_async_copy(fin.at[s, k], out_at(u, core, my_a, my_b), loc.at[s, k])

        def cast_up(u):
            k = u % RING
            rows = out_at(u, core, my_a)
            return remote(rows, rows, up_s.at[s, k], bc_r.at[s, k], up_dev)

        def cast_dn(u):
            k = u % RING
            rows = out_at(u, core, my_a)
            return remote(rows, rows, dn_s.at[s, k], bc_r.at[s, k], dn_dev)

        def aag_copy(u, side):
            k = u % RING
            rows = out_at(u, core, side)
            return remote(rows, rows, aag_s.at[s, k], aag_r.at[s, k], a_dev)

        def p1_copy(u, which):
            k = u % RING
            rows = out_at(u, which, my_a)
            return remote(rows, rows, p1_s.at[s, k], p1_r.at[s, k], pair_dev)

        def p2_copy(u, which):
            k = u % RING
            rows = out_at(u, which, 1 - my_a)
            return remote(rows, rows, p2_s.at[s, k], p2_r.at[s, k], pair_dev)

        def z_send(u, root):
            @pl.when(my_z < root)
            def _():
                up_copy(u).start()

            @pl.when(my_z > root)
            def _():
                dn_copy(u).start()

        def take_below(u):
            k = u % RING
            up_copy(u).wait_recv()
            acc[s, k] = acc[s, k] + rzb[s, k]

        def take_above(u):
            k = u % RING
            dn_copy(u).wait_recv()
            acc[s, k] = acc[s, k] + rza[s, k]

        def stage_first(u):
            a_copy(u).start()

        def stage_pair(u):
            k = u % RING
            root = root_of(u)
            a_copy(u).wait_recv()
            acc[s, k] = part[(u // per_tile) % 2, part_rows(u, my_a)] + ra[s, k]
            a_copy(u).wait_send()

            @pl.when((my_z == 0) | (my_z == top_z))
            def _():
                z_send(u, root)

        def stage_line(level, u):
            root = root_of(u)

            @pl.when((my_z < root) & (my_z == level))
            def _():
                take_below(u)
                up_copy(u).start()

            @pl.when((my_z > root) & (top_z - my_z == level))
            def _():
                take_above(u)
                dn_copy(u).start()

        def stage_root(u):
            @pl.when(my_z == root_of(u))
            def _():
                @pl.when(my_z > 0)
                def _():
                    take_below(u)

                @pl.when(my_z < top_z)
                def _():
                    take_above(u)

                b_copy(u).start()

        def stage_final(u):
            k = u % RING

            @pl.when(my_z == root_of(u))
            def _():
                b_copy(u).wait_recv()
                fin[s, k] = (acc[s, k, b_rows(my_b)] + rb[s, k]) * (1.0 / n_dev)
                bag_copy(u, my_b).start()
                loc_copy(u).start()
                b_copy(u).wait_send()

        def send_on(u, root):
            @pl.when((my_z >= root) & (my_z < top_z))
            def _():
                cast_up(u).start()

            @pl.when((my_z <= root) & (my_z > 0))
            def _():
                cast_dn(u).start()

            aag_copy(u, my_a).start()
            p1_copy(u, core).start()

        def stage_cast(dist, u):
            root = root_of(u)
            if dist == 0:
                @pl.when(my_z == root)
                def _():
                    loc_copy(u).wait()
                    bag_copy(u, my_b).wait_send()
                    bag_copy(u, 1 - my_b).wait_recv()
                    send_on(u, root)
            else:
                @pl.when((my_z == root + dist) | (my_z == root - dist))
                def _():
                    cast_up(u).wait_recv()
                    up_copy(u).wait_send()
                    send_on(u, root)

        def stage_swap(u):
            aag_copy(u, 1 - my_a).wait_recv()
            p2_copy(u, core).start()

        def stage_done(u):
            root = root_of(u)
            p1_copy(u, 1 - core).wait_recv()
            p2_copy(u, 1 - core).wait_recv()

            @pl.when((my_z >= root) & (my_z < top_z))
            def _():
                cast_up(u).wait_send()

            @pl.when((my_z <= root) & (my_z > 0))
            def _():
                cast_dn(u).wait_send()

            aag_copy(u, my_a).wait_send()
            p1_copy(u, core).wait_send()
            p2_copy(u, core).wait_send()

        stages = [stage_first, stage_pair]
        stages += [functools.partial(stage_line, level) for level in range(1, top_z)]
        stages += [stage_root, stage_final]
        stages += [functools.partial(stage_cast, dist) for dist in range(top_z + 1)]
        stages += [stage_swap, stage_done]
        return stages

    streams = [stream_stages(0), stream_stages(1)]
    n_stage = len(streams[0])

    def step(t, carry):
        tile = t // per_tile

        for stage_idx in reversed(range(1, n_stage)):
            u = t - HOP * stage_idx

            @pl.when((u >= 0) & (u < n_unit))
            def _():
                for stages in streams:
                    stages[stage_idx](u)

        @pl.when((t < n_unit) & (t % per_tile == 0))
        def _():
            slot = tile % n_slot
            for copy in factor_copies(slot, tiles[0]):
                copy.wait()
            for lo in range(0, half, 128):
                part[tile % 2, lo:lo + 128, :] = lax.dot_general(
                    fa[slot, :, lo:lo + 128], fb[slot], (((0,), (0,)), ((), ())), preferred_element_type=jnp.float32)

            for later in range(2, n_tile):
                @pl.when(tile + 2 == later)
                def _():
                    for copy in factor_copies(later % n_slot, tiles[later]):
                        copy.start()

        @pl.when(t < n_unit)
        def _():
            for stages in streams:
                stages[0](t)

        return carry

    lax.fori_loop(0, n_unit + HOP * (n_stage - 1), step, 0)


def reduce_tiles(factors, n_tile, n_dev):
    toks = factors[0].shape[0]
    half = WIDTH // 2
    f32, bf16 = jnp.float32, jnp.bfloat16
    dma = pltpu.SemaphoreType.DMA
    slots = pltpu.VMEM((2, RING, 2 * SUB, WIDTH), f32)
    flops = n_tile * 2 * half * 2 * toks * WIDTH
    return pl.pallas_call(
        functools.partial(reduce_kernel, n_tile, n_dev),
        out_shape=jax.ShapeDtypeStruct((n_tile * WIDTH, WIDTH), f32),
        in_specs=[pl.BlockSpec(memory_space=pl.ANY)] * len(factors),
        out_specs=pl.BlockSpec(memory_space=pl.ANY),
        scratch_shapes=[
            pltpu.VMEM((4, 2 * toks, half), bf16),
            pltpu.VMEM((4, 2 * toks, WIDTH), bf16),
            pltpu.VMEM((2, half, WIDTH), f32),
            slots, slots, slots, slots,
            pltpu.VMEM((2, RING, SUB, WIDTH), f32),
            pltpu.VMEM((2, RING, SUB, WIDTH), f32),
        ] + [dma((4,))] * 6 + [dma((2, RING))] * 19,
        compiler_params=pltpu.CompilerParams(collective_id=0, has_side_effects=True, vmem_limit_bytes=48 * 1024 * 1024),
        cost_estimate=pl.CostEstimate(flops=flops, bytes_accessed=n_tile * WIDTH * WIDTH * 8, transcendentals=0),
        name='reduce_tiles',
    )(*factors)


def copy_block(src_ref, dst_ref):
    dst_ref[0] = src_ref[0, 0]


def spread_tiles(tiles, first, count, down=False):
    n_layers = tiles.shape[0]
    shape = (n_layers, count * WIDTH, WIDTH) if down else (n_layers, WIDTH, count * WIDTH)
    return pl.pallas_call(
        copy_block,
        grid=(n_layers, count),
        out_shape=jax.ShapeDtypeStruct(shape, tiles.dtype),
        in_specs=[pl.BlockSpec((1, 1, WIDTH, WIDTH), lambda layer, j: (layer, first + j, 0, 0))],
        out_specs=pl.BlockSpec((1, WIDTH, WIDTH), (lambda layer, j: (layer, j, 0)) if down else (lambda layer, j: (layer, 0, j))),
        name='spread_tiles',
    )(tiles)


def solution(mesh):
    n_dev = mesh.shape['data']

    def local_step(x_loc, grad_y_loc, gain_one, gain_two, w_qkv, w_out, w_up, w_down):
        n_layers = w_qkv.shape[0]
        hidden_x = x_loc
        saved_all = []
        for layer_idx in range(n_layers):
            hidden, act_lo, saved_vals = block_forward(hidden_x, gain_one[layer_idx], gain_two[layer_idx], w_qkv[layer_idx], w_out[layer_idx], w_up[layer_idx])
            saved_all.append(saved_vals)
            if layer_idx + 1 < n_layers:
                hidden_x = hidden + mix_lo('bsf,fd->bsd', act_lo, w_down[layer_idx])
        grad_cur = grad_y_loc
        all_factors = [None] * n_layers
        gain_grads = [None] * (2 * n_layers)
        for layer_idx in reversed(range(n_layers)):
            grad_cur, gain_grads[layer_idx], gain_grads[n_layers + layer_idx], factors = block_backward(grad_cur, saved_all[layer_idx], w_qkv[layer_idx], w_out[layer_idx], w_up[layer_idx], w_down[layer_idx])
            all_factors[layer_idx] = [factor.reshape(factor.shape[1:]) for factor in factors]
        gain_sum = lax.psum(jnp.stack(gain_grads), 'data') / n_dev
        tiles = reduce_tiles([factor for layer in all_factors for factor in layer], n_layers * TILES, n_dev).reshape(n_layers, TILES, WIDTH, WIDTH)

        return (grad_cur, gain_sum[:n_layers], gain_sum[n_layers:], spread_tiles(tiles, 0, 3), spread_tiles(tiles, 3, 1), spread_tiles(tiles, 4, 4),
                spread_tiles(tiles, 8, 4, down=True))

    batch_spec = P('data')
    full_spec = P()
    return jax.shard_map(local_step, mesh=mesh, in_specs=(batch_spec, batch_spec) + (full_spec,) * 6, out_specs=(batch_spec,) + (full_spec,) * 6, check_vma=False)
```

```python
import functools

import jax
import jax.numpy as jnp
from jax import lax
from jax.experimental import pallas as pl
from jax.experimental.pallas import tpu as pltpu
from jax.sharding import PartitionSpec as P

NORM_EPS = 1e-6
HEAD_DIM = 64
WIDTH = 768
TILES = 12
SUB = 16
RING = 16
SPREAD = 8
HOP = 2
MESH_ID = pl.DeviceIdType.MESH


def rms_gain(rows_f, gain_vec):
    return rows_f * lax.rsqrt(jnp.mean(rows_f * rows_f, axis=-1, keepdims=True) + NORM_EPS) * gain_vec


def gelu_tanh(pre_act):
    return jax.nn.gelu(pre_act, approximate=True)


def mix_lo(einsum_spec, lhs_arr, rhs_arr):
    return jnp.einsum(einsum_spec, lhs_arr, rhs_arr, preferred_element_type=jnp.float32).astype(jnp.bfloat16)


def dot_nt(lhs, rhs):
    return lax.dot_general(lhs, rhs, (((1,), (1,)), ((), ())), preferred_element_type=jnp.float32)


def dot_tn(lhs, rhs):
    return lax.dot_general(lhs, rhs, (((0,), (0,)), ((), ())), preferred_element_type=jnp.float32)


def head_probs(q_part, k_pair):
    scores = dot_nt(q_part, k_pair) * HEAD_DIM ** -0.5
    rows = lax.broadcasted_iota(jnp.int32, scores.shape, 0)
    cols = lax.broadcasted_iota(jnp.int32, scores.shape, 1)
    scores = jnp.where(rows >= cols, scores, -1e30)
    weights = jnp.exp(scores - jnp.max(scores, axis=-1, keepdims=True))
    return weights / jnp.sum(weights, axis=-1, keepdims=True)


def pair_masks(shape):
    first = lax.broadcasted_iota(jnp.int32, shape, 1) < HEAD_DIM
    return first, [jnp.where(first, 1.0, 0.0).astype(jnp.bfloat16), jnp.where(first, 0.0, 1.0).astype(jnp.bfloat16)]


def attn_fwd_kernel(q_ref, k_ref, v_ref, o_ref):
    q_pair, k_pair, v_pair = q_ref[...], k_ref[...], v_ref[...]
    first, masks = pair_masks(q_pair.shape)
    outs = [jnp.dot(head_probs(q_pair * mask, k_pair).astype(jnp.bfloat16), v_pair, preferred_element_type=jnp.float32) for mask in masks]
    o_ref[...] = jnp.where(first, outs[0], outs[1]).astype(jnp.bfloat16)


def attn_bwd_kernel(q_ref, k_ref, v_ref, do_ref, dqkv_ref):
    pair = pl.program_id(0)
    q_pair, k_pair, v_pair, do_pair = q_ref[...], k_ref[...], v_ref[...], do_ref[...]
    first, masks = pair_masks(q_pair.shape)
    grads = []
    for mask in masks:
        prob = head_probs(q_pair * mask, k_pair)
        grad_prob = dot_nt(do_pair * mask, v_pair)
        grad_score = (prob * (grad_prob - jnp.sum(prob * grad_prob, axis=-1, keepdims=True)) * HEAD_DIM ** -0.5).astype(jnp.bfloat16)
        grads.append((
            jnp.dot(grad_score, k_pair, preferred_element_type=jnp.float32),
            dot_tn(grad_score, q_pair),
            dot_tn(prob.astype(jnp.bfloat16), do_pair),
        ))
    for part_idx in range(3):
        cols = pl.ds(pl.multiple_of(part_idx * WIDTH + pair * 2 * HEAD_DIM, 2 * HEAD_DIM), 2 * HEAD_DIM)
        dqkv_ref[:, cols] = jnp.where(first, grads[0][part_idx], grads[1][part_idx]).astype(jnp.bfloat16)


def attn_specs(rows, count):
    pairs = WIDTH // (2 * HEAD_DIM)
    return pairs, [pl.BlockSpec((rows, 2 * HEAD_DIM), lambda h, lo=lo * pairs: (0, lo + h)) for lo in range(count)]


def attention(qkv):
    rows = qkv.shape[0]
    pairs, specs = attn_specs(rows, 3)
    return pl.pallas_call(
        attn_fwd_kernel, grid=(pairs,), in_specs=specs, out_specs=attn_specs(rows, 1)[1][0],
        out_shape=jax.ShapeDtypeStruct((rows, WIDTH), jnp.bfloat16), name='attn_fwd',
    )(qkv, qkv, qkv)


def attention_grad(qkv, grad_attn):
    rows = qkv.shape[0]
    pairs, specs = attn_specs(rows, 3)
    return pl.pallas_call(
        attn_bwd_kernel, grid=(pairs,), in_specs=specs + attn_specs(rows, 1)[1], out_specs=pl.BlockSpec((rows, 3 * WIDTH), lambda h: (0, 0)),
        out_shape=jax.ShapeDtypeStruct((rows, 3 * WIDTH), jnp.bfloat16), name='attn_bwd',
    )(qkv, qkv, qkv, grad_attn)


def block_forward(x_blk, gain_a, gain_b, w_qkv, w_out, w_up):
    norm_a, norm_a_back = jax.vjp(rms_gain, x_blk.astype(jnp.float32), gain_a)
    u_one = norm_a.astype(jnp.bfloat16)
    qkv_lo = mix_lo('sd,de->se', u_one, w_qkv)
    attn_out = attention(qkv_lo)
    hidden = x_blk + mix_lo('sd,de->se', attn_out, w_out)
    norm_b, norm_b_back = jax.vjp(rms_gain, hidden.astype(jnp.float32), gain_b)
    u_two = norm_b.astype(jnp.bfloat16)
    pre_lo = mix_lo('sd,df->sf', u_two, w_up)
    act_f, gelu_back = jax.vjp(gelu_tanh, pre_lo.astype(jnp.float32))
    act_lo = act_f.astype(jnp.bfloat16)
    saved_vals = (norm_a_back, u_one, qkv_lo, attn_out, norm_b_back, u_two, gelu_back, act_lo)
    return hidden, act_lo, saved_vals


def block_backward(grad_blk, saved_vals, w_qkv, w_out, w_up, w_down):
    (norm_a_back, u_one, qkv_lo, attn_out, norm_b_back, u_two, gelu_back, act_lo) = saved_vals
    grad_act = mix_lo('sd,fd->sf', grad_blk, w_down)
    (grad_pre_f,) = gelu_back(grad_act.astype(jnp.float32))
    grad_pre = grad_pre_f.astype(jnp.bfloat16)
    grad_u_two = mix_lo('sf,df->sd', grad_pre, w_up)
    grad_h_norm, grad_gain_b = norm_b_back(grad_u_two.astype(jnp.float32))
    grad_hidden = (grad_blk.astype(jnp.float32) + grad_h_norm).astype(jnp.bfloat16)
    grad_attn = mix_lo('se,de->sd', grad_hidden, w_out)
    grad_qkv = attention_grad(qkv_lo, grad_attn)
    grad_u_one = mix_lo('se,de->sd', grad_qkv, w_qkv)
    grad_x_norm, grad_gain_a = norm_a_back(grad_u_one.astype(jnp.float32))
    grad_x_blk = (grad_hidden.astype(jnp.float32) + grad_x_norm).astype(jnp.bfloat16)
    factors = (u_one, grad_qkv, attn_out, grad_hidden, u_two, grad_pre, act_lo, grad_blk)
    return grad_x_blk, grad_gain_a, grad_gain_b, factors


def layer_tiles(factors):
    u_one, grad_qkv, attn_out, grad_hidden, u_two, grad_pre, act_lo, grad_blk = factors
    tiles = []
    for lhs, rhs in ((u_one, grad_qkv), (attn_out, grad_hidden), (u_two, grad_pre), (act_lo, grad_blk)):
        tiles += [(lhs, left, rhs, right) for left in range(0, lhs.shape[1], WIDTH) for right in range(0, rhs.shape[1], WIDTH)]
    return tiles


def reduce_kernel(n_tile, n_dev, *refs):
    n_factor = 8 * (-(-n_tile // TILES))
    reduce_body(n_tile, n_dev, refs[:n_factor], *refs[n_factor:])


def reduce_body(n_tile, n_dev, f_refs, gain_ref, g_ref, gain_out, gs, gr, gz, gs_s, gs_r, gz_s, gz_r, fa, fb, part, ra, acc, rzb, rza, rb, fin,
                  fl_a, fl_b, fs_a, fs_b, fr_a, fr_b,
                  ra_s, ra_r, z_s, zb_r, za_r, b_s, b_r, bag_s, bag_r, loc, bc_r, up_s, dn_s, aag_s, aag_r, p1_s, p1_r, p2_s, p2_r):
    toks = f_refs[0].shape[0]
    half = WIDTH // 2
    n_slot = fa.shape[0]
    tiles = [tile for lo in range(0, len(f_refs), 8) for tile in layer_tiles(f_refs[lo:lo + 8])][:n_tile]
    per_tile = half // (8 * SUB)
    n_unit = n_tile * per_tile
    me = lax.axis_index('data')
    core, my_x, my_y, my_z = me % 2, (me // 2) % 2, (me // 4) % 2, me // 8
    top_z = n_dev // 8 - 1
    x_dev, y_dev, pair_dev = me + 2 - 4 * my_x, me + 4 - 8 * my_y, me + 1 - 2 * core
    up_dev, dn_dev = me + 8, me - 8

    barrier = pltpu.get_barrier_semaphore()
    for dev in (x_dev, y_dev, pair_dev):
        pl.semaphore_signal(barrier, inc=1, device_id=(dev,), device_id_type=MESH_ID)

    z_devs = [me + 8 * ((my_z + dist) % (top_z + 1) - my_z) for dist in range(1, top_z + 1)]
    for dev in z_devs:
        pl.semaphore_signal(barrier, inc=1, device_id=(dev,), device_id_type=MESH_ID)
    pl.semaphore_wait(barrier, 3 + top_z)

    def remote(src, dst, send_sem, recv_sem, dev):
        return pltpu.make_async_remote_copy(src_ref=src, dst_ref=dst, send_sem=send_sem, recv_sem=recv_sem, device_id=(dev,), device_id_type=MESH_ID)

    def factor_copies(slot, source):
        lhs, left, rhs, right = source
        mine = pl.ds(pl.multiple_of(left + core * half, 128), half)
        other = pl.ds(pl.multiple_of(left + (1 - core) * half, 128), half)
        lo, hi = pl.ds(0, toks), pl.ds(toks, toks)
        cols = pl.ds(right, WIDTH)
        return (
            pltpu.make_async_copy(lhs.at[:, mine], fa.at[slot, lo], fl_a.at[slot]),
            pltpu.make_async_copy(rhs.at[:, cols], fb.at[slot, lo], fl_b.at[slot]),
            remote(lhs.at[:, other], fa.at[slot, hi], fs_a.at[slot], fr_a.at[slot], pair_dev),
            remote(rhs.at[:, cols], fb.at[slot, hi], fs_b.at[slot], fr_b.at[slot], pair_dev),
        )

    for tile in range(2):
        for copy in factor_copies(tile, tiles[tile]):
            copy.start()

    def stream_stages(s):
        my_a, my_b = (my_x, my_y) if s == 0 else (my_y, my_x)
        a_dev, b_dev = (x_dev, y_dev) if s == 0 else (y_dev, x_dev)

        def root_of(u):
            return (u + 2 * s) % (top_z + 1)

        def part_rows(u, side):
            return pl.ds(pl.multiple_of((u % per_tile) * (8 * SUB) + s * (4 * SUB) + side * (2 * SUB), 8), 2 * SUB)

        def part_at(u, side):
            return part.at[(u // per_tile) % 2, part_rows(u, side)]

        def out_at(u, which, side, b_side=None):
            base = (u // per_tile) * WIDTH + which * half + (u % per_tile) * (8 * SUB) + s * (4 * SUB) + side * (2 * SUB)
            if b_side is None:
                return g_ref.at[pl.ds(pl.multiple_of(base, 8), 2 * SUB)]
            return g_ref.at[pl.ds(pl.multiple_of(base + b_side * SUB, 8), SUB)]

        def a_copy(u):
            k = u % RING
            return remote(part_at(u, 1 - my_a), ra.at[s, k], ra_s.at[s, k], ra_r.at[s, k], a_dev)

        def up_copy(u):
            k = u % RING
            return remote(acc.at[s, k], rzb.at[s, k], z_s.at[s, k], zb_r.at[s, k], up_dev)

        def dn_copy(u):
            k = u % RING
            return remote(acc.at[s, k], rza.at[s, k], z_s.at[s, k], za_r.at[s, k], dn_dev)

        def b_rows(side):
            return pl.ds(pl.multiple_of(side * SUB, 8), SUB)

        def b_copy(u):
            k = u % RING
            return remote(acc.at[s, k, b_rows(1 - my_b)], rb.at[s, k], b_s.at[s, k], b_r.at[s, k], b_dev)

        def bag_copy(u, b_side):
            k = u % RING
            return remote(fin.at[s, k], out_at(u, core, my_a, b_side), bag_s.at[s, k], bag_r.at[s, k], b_dev)

        def loc_copy(u):
            k = u % RING
            return pltpu.make_async_copy(fin.at[s, k], out_at(u, core, my_a, my_b), loc.at[s, k])

        def cast_up(u):
            k = u % RING
            rows = out_at(u, core, my_a)
            return remote(rows, rows, up_s.at[s, k], bc_r.at[s, k], up_dev)

        def cast_dn(u):
            k = u % RING
            rows = out_at(u, core, my_a)
            return remote(rows, rows, dn_s.at[s, k], bc_r.at[s, k], dn_dev)

        def aag_copy(u, side):
            k = u % RING
            rows = out_at(u, core, side)
            return remote(rows, rows, aag_s.at[s, k], aag_r.at[s, k], a_dev)

        def p1_copy(u, which):
            k = u % RING
            rows = out_at(u, which, my_a)
            return remote(rows, rows, p1_s.at[s, k], p1_r.at[s, k], pair_dev)

        def p2_copy(u, which):
            k = u % RING
            rows = out_at(u, which, 1 - my_a)
            return remote(rows, rows, p2_s.at[s, k], p2_r.at[s, k], pair_dev)

        def z_send(u, root):
            @pl.when(my_z < root)
            def _():
                up_copy(u).start()

            @pl.when(my_z > root)
            def _():
                dn_copy(u).start()

        def take_below(u):
            k = u % RING
            up_copy(u).wait_recv()
            acc[s, k] = acc[s, k] + rzb[s, k]

        def take_above(u):
            k = u % RING
            dn_copy(u).wait_recv()
            acc[s, k] = acc[s, k] + rza[s, k]

        def stage_first(u):
            a_copy(u).start()

        def stage_pair(u):
            k = u % RING
            root = root_of(u)
            a_copy(u).wait_recv()
            acc[s, k] = part[(u // per_tile) % 2, part_rows(u, my_a)] + ra[s, k]
            a_copy(u).wait_send()

            @pl.when((my_z == 0) | (my_z == top_z))
            def _():
                z_send(u, root)

        def stage_line(level, u):
            root = root_of(u)

            @pl.when((my_z < root) & (my_z == level))
            def _():
                take_below(u)
                up_copy(u).start()

            @pl.when((my_z > root) & (top_z - my_z == level))
            def _():
                take_above(u)
                dn_copy(u).start()

        def stage_root(u):
            @pl.when(my_z == root_of(u))
            def _():
                @pl.when(my_z > 0)
                def _():
                    take_below(u)

                @pl.when(my_z < top_z)
                def _():
                    take_above(u)

                b_copy(u).start()

        def stage_final(u):
            k = u % RING

            @pl.when(my_z == root_of(u))
            def _():
                b_copy(u).wait_recv()
                fin[s, k] = (acc[s, k, b_rows(my_b)] + rb[s, k]) * (1.0 / n_dev)
                bag_copy(u, my_b).start()
                loc_copy(u).start()
                b_copy(u).wait_send()

        def send_on(u, root):
            @pl.when((my_z >= root) & (my_z < top_z))
            def _():
                cast_up(u).start()

            @pl.when((my_z <= root) & (my_z > 0))
            def _():
                cast_dn(u).start()

            aag_copy(u, my_a).start()
            p1_copy(u, core).start()

        def stage_cast(dist, u):
            root = root_of(u)
            if dist == 0:
                @pl.when(my_z == root)
                def _():
                    loc_copy(u).wait()
                    bag_copy(u, my_b).wait_send()
                    bag_copy(u, 1 - my_b).wait_recv()
                    send_on(u, root)
            else:
                @pl.when((my_z == root + dist) | (my_z == root - dist))
                def _():
                    cast_up(u).wait_recv()
                    up_copy(u).wait_send()
                    send_on(u, root)

        def stage_swap(u):
            aag_copy(u, 1 - my_a).wait_recv()
            p2_copy(u, core).start()

        def stage_done(u):
            root = root_of(u)
            p1_copy(u, 1 - core).wait_recv()
            p2_copy(u, 1 - core).wait_recv()

            @pl.when((my_z >= root) & (my_z < top_z))
            def _():
                cast_up(u).wait_send()

            @pl.when((my_z <= root) & (my_z > 0))
            def _():
                cast_dn(u).wait_send()

            aag_copy(u, my_a).wait_send()
            p1_copy(u, core).wait_send()
            p2_copy(u, core).wait_send()

        stages = [stage_first, stage_pair]
        stages += [functools.partial(stage_line, level) for level in range(1, top_z)]
        stages += [stage_root, stage_final]
        stages += [functools.partial(stage_cast, dist) for dist in range(top_z + 1)]
        stages += [stage_swap, stage_done]
        return stages

    gain_devs = (pair_dev, x_dev, y_dev)

    def gain_copy(hop):
        return remote(gs.at[hop], gr.at[hop], gs_s.at[hop], gs_r.at[hop], gain_devs[hop])

    def gain_line(dist, slot):
        return remote(gs.at[3], gz.at[slot], gz_s.at[dist], gz_r.at[slot], z_devs[dist])

    def gain_steps(t):
        @pl.when(t == 0)
        def _():
            gs[0] = gain_ref[...]
            gain_copy(0).start()

        for hop in range(1, 4):
            @pl.when(t == 4 * hop)
            def _():
                gain_copy(hop - 1).wait()
                gs[hop] = gs[hop - 1] + gr[hop - 1]
                if hop < 3:
                    gain_copy(hop).start()
                else:
                    gz[my_z] = gs[hop]
                    for dist in range(top_z):
                        gain_line(dist, my_z).start()

        @pl.when(t == 16)
        def _():
            for dist in range(top_z):
                gain_line(dist, my_z).wait_send()
                gain_line(dist, (my_z + dist + 1) % (top_z + 1)).wait_recv()
            total = gz[0]
            for slot in range(1, top_z + 1):
                total = total + gz[slot]
            gain_out[...] = total * (1.0 / n_dev)

    streams = [stream_stages(0), stream_stages(1)]
    n_stage = len(streams[0])

    def step(t, carry):
        tile = t // per_tile
        gain_steps(t)

        for stage_idx in reversed(range(1, n_stage)):
            u = t - HOP * stage_idx

            @pl.when((u >= 0) & (u < n_unit))
            def _():
                for stages in streams:
                    stages[stage_idx](u)

        @pl.when((t < n_unit) & (t % per_tile == 0))
        def _():
            slot = tile % n_slot
            for copy in factor_copies(slot, tiles[0]):
                copy.wait()
            for lo in range(0, half, 128):
                part[tile % 2, lo:lo + 128, :] = lax.dot_general(
                    fa[slot, :, lo:lo + 128], fb[slot], (((0,), (0,)), ((), ())), preferred_element_type=jnp.float32)

            for later in range(2, n_tile):
                @pl.when(tile + 2 == later)
                def _():
                    for copy in factor_copies(later % n_slot, tiles[later]):
                        copy.start()

        @pl.when(t < n_unit)
        def _():
            for stages in streams:
                stages[0](t)

        return carry

    lax.fori_loop(0, n_unit + HOP * (n_stage - 1), step, 0)


def reduce_tiles(factors, gains, n_tile, n_dev):
    toks = factors[0].shape[0]
    half = WIDTH // 2
    f32, bf16 = jnp.float32, jnp.bfloat16
    dma = pltpu.SemaphoreType.DMA
    slots = pltpu.VMEM((2, RING, 2 * SUB, WIDTH), f32)
    flops = n_tile * 2 * half * 2 * toks * WIDTH
    return pl.pallas_call(
        functools.partial(reduce_kernel, n_tile, n_dev),
        out_shape=(jax.ShapeDtypeStruct((n_tile * WIDTH, WIDTH), f32), jax.ShapeDtypeStruct(gains.shape, f32)),
        in_specs=[pl.BlockSpec(memory_space=pl.ANY)] * len(factors) + [pl.BlockSpec(memory_space=pltpu.VMEM)],
        out_specs=(pl.BlockSpec(memory_space=pl.ANY), pl.BlockSpec(memory_space=pltpu.VMEM)),
        scratch_shapes=[
            pltpu.VMEM((4,) + gains.shape, f32),
            pltpu.VMEM((3,) + gains.shape, f32),
            pltpu.VMEM((n_dev // 8,) + gains.shape, f32),
            dma((3,)), dma((3,)), dma((n_dev // 8 - 1,)), dma((n_dev // 8,)),
            pltpu.VMEM((4, 2 * toks, half), bf16),
            pltpu.VMEM((4, 2 * toks, WIDTH), bf16),
            pltpu.VMEM((2, half, WIDTH), f32),
            slots, slots, slots, slots,
            pltpu.VMEM((2, RING, SUB, WIDTH), f32),
            pltpu.VMEM((2, RING, SUB, WIDTH), f32),
        ] + [dma((4,))] * 6 + [dma((2, RING))] * 19,
        compiler_params=pltpu.CompilerParams(collective_id=0, has_side_effects=True, vmem_limit_bytes=48 * 1024 * 1024),
        cost_estimate=pl.CostEstimate(flops=flops, bytes_accessed=n_tile * WIDTH * WIDTH * 8, transcendentals=0),
        name='reduce_tiles',
    )(*factors, gains)


def spread_kernel(n_layers, src_ref, qkv_ref, out_ref, up_ref, down_ref, buf, read_sem, write_sem):
    moves = []
    for layer in range(n_layers):
        for j in range(TILES):
            if j < 3:
                dst = qkv_ref.at[layer, :, pl.ds(j * WIDTH, WIDTH)]
            elif j < 4:
                dst = out_ref.at[layer]
            elif j < 8:
                dst = up_ref.at[layer, :, pl.ds((j - 4) * WIDTH, WIDTH)]
            else:
                dst = down_ref.at[layer, pl.ds((j - 8) * WIDTH, WIDTH)]
            slot = len(moves) % SPREAD
            moves.append((pltpu.make_async_copy(src_ref.at[pl.ds((layer * TILES + j) * WIDTH, WIDTH)], buf.at[slot], read_sem.at[slot]),
                          pltpu.make_async_copy(buf.at[slot], dst, write_sem.at[slot])))
    ahead = SPREAD // 2
    for read, _ in moves[:ahead]:
        read.start()
    for idx, (read, write) in enumerate(moves):
        if idx >= ahead:
            moves[idx - ahead][1].wait()
        if idx + ahead < len(moves):
            moves[idx + ahead][0].start()
        read.wait()
        write.start()
    for _, write in moves[-ahead:]:
        write.wait()


def spread_tiles(tiles, n_layers):
    f32 = jnp.float32
    anyspace = pl.BlockSpec(memory_space=pl.ANY)
    shapes = ((WIDTH, 3 * WIDTH), (WIDTH, WIDTH), (WIDTH, 4 * WIDTH), (4 * WIDTH, WIDTH))
    return pl.pallas_call(
        functools.partial(spread_kernel, n_layers),
        out_shape=tuple(jax.ShapeDtypeStruct((n_layers,) + shape, f32) for shape in shapes),
        in_specs=[anyspace],
        out_specs=(anyspace,) * 4,
        scratch_shapes=[pltpu.VMEM((SPREAD, WIDTH, WIDTH), f32), pltpu.SemaphoreType.DMA((SPREAD,)), pltpu.SemaphoreType.DMA((SPREAD,))],
        compiler_params=pltpu.CompilerParams(vmem_limit_bytes=32 * 1024 * 1024),
        name='spread_tiles',
    )(tiles)


def solution(mesh):
    n_dev = mesh.shape['data']

    def local_step(x_loc, grad_y_loc, gain_one, gain_two, w_qkv, w_out, w_up, w_down):
        n_layers = w_qkv.shape[0]
        hidden_x = x_loc[0]
        saved_all = []
        for layer_idx in range(n_layers):
            hidden, act_lo, saved_vals = block_forward(hidden_x, gain_one[layer_idx], gain_two[layer_idx], w_qkv[layer_idx], w_out[layer_idx], w_up[layer_idx])
            saved_all.append(saved_vals)
            if layer_idx + 1 < n_layers:
                hidden_x = hidden + mix_lo('sf,fd->sd', act_lo, w_down[layer_idx])
        grad_cur = grad_y_loc[0]
        all_factors = [None] * n_layers
        gain_grads = [None] * (2 * n_layers)
        for layer_idx in reversed(range(n_layers)):
            grad_cur, gain_grads[layer_idx], gain_grads[n_layers + layer_idx], all_factors[layer_idx] = block_backward(grad_cur, saved_all[layer_idx], w_qkv[layer_idx], w_out[layer_idx], w_up[layer_idx], w_down[layer_idx])
        gains = jnp.stack(gain_grads + [jnp.zeros_like(gain_grads[0])] * (-2 * n_layers % 8))
        tiles, gain_sum = reduce_tiles([factor for layer in all_factors for factor in layer], gains, n_layers * TILES, n_dev)
        return (grad_cur[None], gain_sum[:n_layers], gain_sum[n_layers:2 * n_layers]) + tuple(spread_tiles(tiles, n_layers))

    batch_spec = P('data')
    full_spec = P()
    return jax.shard_map(local_step, mesh=mesh, in_specs=(batch_spec, batch_spec) + (full_spec,) * 6, out_specs=(batch_spec,) + (full_spec,) * 6, check_vma=False)
```

```python
import functools
import math

import jax
import jax.numpy as jnp
from jax import lax
from jax.experimental import pallas as pl
from jax.experimental.pallas import tpu as pltpu
from jax.sharding import PartitionSpec as P

NORM_EPS = 1e-6
HEAD_DIM = 64
WIDTH = 768
TILES = 12
SUB = 16
RING = 16
SPREAD = 8
PIECES = 12
HOP = 2
MESH_ID = pl.DeviceIdType.MESH


def rms_gain(rows_f, gain_vec):
    return rows_f * lax.rsqrt(jnp.mean(rows_f * rows_f, axis=-1, keepdims=True) + NORM_EPS) * gain_vec


def gelu_tanh(pre_act):
    return jax.nn.gelu(pre_act, approximate=True)


def mix_lo(einsum_spec, lhs_arr, rhs_arr):
    return jnp.einsum(einsum_spec, lhs_arr, rhs_arr, preferred_element_type=jnp.float32).astype(jnp.bfloat16)


def dot_nt(lhs, rhs):
    return lax.dot_general(lhs, rhs, (((1,), (1,)), ((), ())), preferred_element_type=jnp.float32)


def dot_tn(lhs, rhs):
    return lax.dot_general(lhs, rhs, (((0,), (0,)), ((), ())), preferred_element_type=jnp.float32)


def head_probs(q_part, k_pair):
    scores = dot_nt(q_part, k_pair) * HEAD_DIM ** -0.5
    rows = lax.broadcasted_iota(jnp.int32, scores.shape, 0)
    cols = lax.broadcasted_iota(jnp.int32, scores.shape, 1)
    scores = jnp.where(rows >= cols, scores, -1e30)
    weights = jnp.exp(scores - jnp.max(scores, axis=-1, keepdims=True))
    return weights / jnp.sum(weights, axis=-1, keepdims=True)


def pair_masks(shape):
    first = lax.broadcasted_iota(jnp.int32, shape, 1) < HEAD_DIM
    return first, [jnp.where(first, 1.0, 0.0).astype(jnp.bfloat16), jnp.where(first, 0.0, 1.0).astype(jnp.bfloat16)]


def attn_fwd_kernel(q_ref, k_ref, v_ref, o_ref):
    q_pair, k_pair, v_pair = q_ref[...], k_ref[...], v_ref[...]
    first, masks = pair_masks(q_pair.shape)
    outs = [jnp.dot(head_probs(q_pair * mask, k_pair).astype(jnp.bfloat16), v_pair, preferred_element_type=jnp.float32) for mask in masks]
    o_ref[...] = jnp.where(first, outs[0], outs[1]).astype(jnp.bfloat16)


def pair_grads(q_pair, k_pair, v_pair, do_pair):
    first, masks = pair_masks(q_pair.shape)
    grads = []
    for mask in masks:
        prob = head_probs(q_pair * mask, k_pair)
        grad_prob = dot_nt(do_pair * mask, v_pair)
        grad_score = (prob * (grad_prob - jnp.sum(prob * grad_prob, axis=-1, keepdims=True)) * HEAD_DIM ** -0.5).astype(jnp.bfloat16)
        grads.append((
            jnp.dot(grad_score, k_pair, preferred_element_type=jnp.float32),
            dot_tn(grad_score, q_pair),
            dot_tn(prob.astype(jnp.bfloat16), do_pair),
        ))
    return [jnp.where(first, grads[0][idx], grads[1][idx]).astype(jnp.bfloat16) for idx in range(3)]


def attn_bwd_kernel(q_ref, k_ref, v_ref, do_ref, dqkv_ref):
    pair = pair_grads(q_ref[...], k_ref[...], v_ref[...], do_ref[...])
    for part_idx in range(3):
        cols = pl.ds(pl.multiple_of(part_idx * WIDTH + pl.program_id(0) * 2 * HEAD_DIM, 2 * HEAD_DIM), 2 * HEAD_DIM)
        dqkv_ref[:, cols] = pair[part_idx]


def attn_specs(rows, count):
    pairs = WIDTH // (2 * HEAD_DIM)
    return pairs, [pl.BlockSpec((rows, 2 * HEAD_DIM), lambda h, lo=lo * pairs: (0, lo + h)) for lo in range(count)]


def attention(qkv):
    rows = qkv.shape[0]
    pairs, specs = attn_specs(rows, 3)
    return pl.pallas_call(
        attn_fwd_kernel, grid=(pairs,), in_specs=specs, out_specs=attn_specs(rows, 1)[1][0],
        out_shape=jax.ShapeDtypeStruct((rows, WIDTH), jnp.bfloat16), name='attn_fwd',
    )(qkv, qkv, qkv)


def attention_grad(qkv, grad_attn):
    rows = qkv.shape[0]
    pairs, specs = attn_specs(rows, 3)
    return pl.pallas_call(
        attn_bwd_kernel, grid=(pairs,), in_specs=specs + attn_specs(rows, 1)[1], out_specs=pl.BlockSpec((rows, 3 * WIDTH), lambda h: (0, 0)),
        out_shape=jax.ShapeDtypeStruct((rows, 3 * WIDTH), jnp.bfloat16), name='attn_bwd',
    )(qkv, qkv, qkv, grad_attn)


def block_forward(x_blk, gain_a, gain_b, w_qkv, w_out, w_up):
    norm_a, norm_a_back = jax.vjp(rms_gain, x_blk.astype(jnp.float32), gain_a)
    u_one = norm_a.astype(jnp.bfloat16)
    qkv_lo = mix_lo('sd,de->se', u_one, w_qkv)
    attn_out = attention(qkv_lo)
    hidden = x_blk + mix_lo('sd,de->se', attn_out, w_out)
    norm_b, norm_b_back = jax.vjp(rms_gain, hidden.astype(jnp.float32), gain_b)
    u_two = norm_b.astype(jnp.bfloat16)
    pre_lo = mix_lo('sd,df->sf', u_two, w_up)
    act_f, gelu_back = jax.vjp(gelu_tanh, pre_lo.astype(jnp.float32))
    act_lo = act_f.astype(jnp.bfloat16)
    saved_vals = (norm_a_back, u_one, qkv_lo, attn_out, norm_b_back, u_two, gelu_back, act_lo)
    return hidden, act_lo, saved_vals, (u_one, attn_out, u_two, act_lo), (x_blk, hidden, pre_lo, qkv_lo)


def block_backward(grad_blk, saved_vals, w_qkv, w_out, w_up, w_down):
    (norm_a_back, u_one, qkv_lo, attn_out, norm_b_back, u_two, gelu_back, act_lo) = saved_vals
    grad_act = mix_lo('sd,fd->sf', grad_blk, w_down)
    (grad_pre_f,) = gelu_back(grad_act.astype(jnp.float32))
    grad_pre = grad_pre_f.astype(jnp.bfloat16)
    grad_u_two = mix_lo('sf,df->sd', grad_pre, w_up)
    grad_h_norm, grad_gain_b = norm_b_back(grad_u_two.astype(jnp.float32))
    grad_hidden = (grad_blk.astype(jnp.float32) + grad_h_norm).astype(jnp.bfloat16)
    grad_attn = mix_lo('se,de->sd', grad_hidden, w_out)
    grad_qkv = attention_grad(qkv_lo, grad_attn)
    grad_u_one = mix_lo('se,de->sd', grad_qkv, w_qkv)
    grad_x_norm, grad_gain_a = norm_a_back(grad_u_one.astype(jnp.float32))
    grad_x_blk = (grad_hidden.astype(jnp.float32) + grad_x_norm).astype(jnp.bfloat16)
    factors = (u_one, grad_qkv, attn_out, grad_hidden, u_two, grad_pre, act_lo, grad_blk)
    return grad_x_blk, grad_gain_a, grad_gain_b, factors


def layer_tiles(factors):
    u_one, grad_qkv, attn_out, grad_hidden, u_two, grad_pre, act_lo, grad_blk = factors
    tiles = []
    for lhs, rhs in ((u_one, grad_qkv), (attn_out, grad_hidden), (u_two, grad_pre), (act_lo, grad_blk)):
        tiles += [(lhs, left, rhs, right) for left in range(0, lhs.shape[1], WIDTH) for right in range(0, rhs.shape[1], WIDTH)]
    return tiles


def norm_grad(rows, gain, grad_out):
    scale = lax.rsqrt(jnp.mean(rows * rows, axis=-1, keepdims=True) + NORM_EPS)
    grad_gain = jnp.sum(grad_out * rows * scale, axis=0, keepdims=True)
    grad_unit = grad_out * gain
    grad_rows = grad_unit * scale - rows * (scale * scale * scale) * jnp.mean(rows * grad_unit, axis=-1, keepdims=True)
    return grad_rows, grad_gain


def gelu_slope(z):
    const = (2.0 / math.pi) ** 0.5
    curve = jnp.tanh(const * (z + 0.044715 * (z * z * z)))
    return 0.5 * (1.0 + curve) + 0.5 * z * (1.0 - curve * curve) * const * (1.0 + 3.0 * 0.044715 * (z * z))


def backward_pieces(n_layers, saved, weights, gain_one, gain_two, grads_hbm, dx_hbm, grad_x, gs, vm, load, store):
    w_qkv, w_out, w_up, w_down = weights
    dqkv_hbm, dh_hbm, dz_hbm = grads_hbm
    w2, w1, zb, hb, wo, qkvb, wq, xb, dz, dh, dqkv, dy, do, acc = vm
    n_low = n_layers - 1

    def cols(j):
        return pl.ds(pl.multiple_of(j * WIDTH, WIDTH), WIDTH)

    def weight_loads(low, j):
        layer, slot = n_layers - 2 - low, j % 2
        return (pltpu.make_async_copy(w_down.at[layer, cols(j)], w2.at[slot], load.at[slot]),
                pltpu.make_async_copy(w_up.at[layer, :, cols(j)], w1.at[slot], load.at[2 + slot]))

    def saved_load(kind, low, src_cols, dst, sem, act):
        for which in range(n_low):
            src = saved[which][kind] if src_cols is None else saved[which][kind].at[:, src_cols]

            @pl.when(low == which)
            def _():
                getattr(pltpu.make_async_copy(src, dst, sem), act)()

    def mlp_loads(low, j, act):
        for copy in weight_loads(low, j):
            getattr(copy, act)()
        saved_load(2, low, cols(j), zb.at[j % 2], load.at[4 + j % 2], act)

    def attn_loads(low, act):
        getattr(pltpu.make_async_copy(w_out.at[n_layers - 2 - low], wo, load.at[6]), act)()
        saved_load(1, low, None, hb, load.at[7], act)

    def last_loads(low, act):
        getattr(pltpu.make_async_copy(w_qkv.at[n_layers - 2 - low], wq, load.at[9]), act)()
        saved_load(0, low, None, xb, load.at[10], act)

    def add_gain(row, value):
        rows = lax.broadcasted_iota(jnp.int32, gs.shape[1:], 0)
        gs[0] = gs[0] + jnp.where(rows == row, value, 0.0)

    def prologue():
        first = pltpu.make_async_copy(dx_hbm[0], dy, load.at[11])
        first.start()
        mlp_loads(jnp.int32(0), jnp.int32(0), 'start')
        first.wait()

    def dz_out(low, j):
        return pltpu.make_async_copy(dz.at[:, cols(j)], dz_hbm.at[low, :, cols(j)], store.at[j])

    def piece(t):
        low, p = (t - 1) // PIECES, (t - 1) % PIECES
        layer = n_layers - 2 - low
        active = (t >= 1) & (t <= n_low * PIECES)

        @pl.when(active & (p < 4))
        def _():
            mlp_loads(low, p, 'wait')

            @pl.when(p < 3)
            def _():
                mlp_loads(low, p + 1, 'start')

            @pl.when(p == 3)
            def _():
                attn_loads(low, 'start')
                saved_load(3, low, None, qkvb, load.at[8], 'start')

            slot = p % 2
            grad_act = dot_nt(dy[...], w2[slot]).astype(jnp.bfloat16).astype(jnp.float32)
            grad_pre = (gelu_slope(zb[slot].astype(jnp.float32)) * grad_act).astype(jnp.bfloat16)
            dz[:, cols(p)] = grad_pre
            term = dot_nt(grad_pre, w1[slot])

            @pl.when(p == 0)
            def _():
                acc[...] = term

            @pl.when(p > 0)
            def _():
                acc[...] = acc[...] + term

            dz_out(low, p).start()

        @pl.when(active & (p == 4))
        def _():
            attn_loads(low, 'wait')
            last_loads(low, 'start')
            grad_out = acc[...].astype(jnp.bfloat16).astype(jnp.float32)
            gain = gain_two[pl.ds(layer, 1), :]
            grad_rows, grad_gain = norm_grad(hb[...].astype(jnp.float32), gain, grad_out)
            dh[...] = (dy[...].astype(jnp.float32) + grad_rows).astype(jnp.bfloat16)
            add_gain(n_layers + layer, grad_gain)
            do[...] = dot_nt(dh[...], wo[...]).astype(jnp.bfloat16)
            pltpu.make_async_copy(dh, dh_hbm.at[low], store.at[4]).start()
            saved_load(3, low, None, qkvb, load.at[8], 'wait')
            for j in range(4):
                dz_out(low, j).wait()

        @pl.when(active & (p >= 5) & (p < 11))
        def _():
            def pair_cols(part_idx):
                return pl.ds(pl.multiple_of(part_idx * WIDTH + (p - 5) * 2 * HEAD_DIM, 2 * HEAD_DIM), 2 * HEAD_DIM)

            pair = pair_grads(qkvb[:, pair_cols(0)], qkvb[:, pair_cols(1)], qkvb[:, pair_cols(2)], do[:, pair_cols(0)])
            for part_idx in range(3):
                dqkv[:, pair_cols(part_idx)] = pair[part_idx]

        @pl.when(active & (p == 11))
        def _():
            last_loads(low, 'wait')
            dqkv_out = pltpu.make_async_copy(dqkv, dqkv_hbm.at[low], store.at[5])
            dqkv_out.start()

            @pl.when(low + 1 < n_low)
            def _():
                mlp_loads(low + 1, jnp.int32(0), 'start')

            grad_out = dot_nt(dqkv[...], wq[...]).astype(jnp.bfloat16).astype(jnp.float32)
            gain = gain_one[pl.ds(layer, 1), :]
            grad_rows, grad_gain = norm_grad(xb[...].astype(jnp.float32), gain, grad_out)
            add_gain(layer, grad_gain)
            dy[...] = (dh[...].astype(jnp.float32) + grad_rows).astype(jnp.bfloat16)
            for which in range(n_low):
                dst = grad_x if which == n_low - 1 else dx_hbm[which + 1]

                @pl.when(low == which)
                def _():
                    out = pltpu.make_async_copy(dy, dst, store.at[6])
                    out.start()
                    out.wait()

            pltpu.make_async_copy(dh, dh_hbm.at[low], store.at[4]).wait()
            dqkv_out.wait()

    return prologue, piece


def reduce_kernel(n_layers, n_tile, n_dev, *refs):
    refs = list(refs)

    def take(count):
        out = refs[:count]
        del refs[:count]
        return out

    n_low = n_layers - 1
    top = take(8)
    lower = [take(4) for _ in range(n_low)]
    saved = [take(4) for _ in range(n_low)]
    weights = take(4)
    gain_one, gain_two, gain_ref, dx_top = take(4)
    g_ref, gain_out, grad_x, dqkv_hbm, dh_hbm, dz_hbm, dx_mid = take(7)
    dx_hbm = [dx_top] + [dx_mid.at[which] for which in range(n_low - 1)]
    gs, *vm = take(15)
    load, store = take(2)
    prologue, piece = backward_pieces(n_layers, saved, weights, gain_one, gain_two, (dqkv_hbm, dh_hbm, dz_hbm), dx_hbm, grad_x, gs, vm, load, store)
    f_refs = list(top)
    for low in range(n_low):
        u_one, attn_out, u_two, act_lo = lower[low]
        f_refs += [u_one, dqkv_hbm.at[low], attn_out, dh_hbm.at[low], u_two, dz_hbm.at[low], act_lo, dx_hbm[low]]
    reduce_body(n_tile, n_dev, prologue, piece, n_low * PIECES + 2, f_refs, gain_ref, g_ref, gain_out, gs, *refs)


def reduce_body(n_tile, n_dev, prologue, piece, gain_start, f_refs, gain_ref, g_ref, gain_out, gs, gr, gz, gs_s, gs_r, gz_s, gz_r, fa, fb, part, ra, acc, rzb, rza, rb, fin,
                fl_a, fl_b, fs_a, fs_b, fr_a, fr_b,
                ra_s, ra_r, z_s, zb_r, za_r, b_s, b_r, bag_s, bag_r, loc, bc_r, up_s, dn_s, aag_s, aag_r, p1_s, p1_r, p2_s, p2_r):
    toks = f_refs[0].shape[0]
    half = WIDTH // 2
    n_slot = fa.shape[0]
    tiles = [tile for lo in range(0, len(f_refs), 8) for tile in layer_tiles(f_refs[lo:lo + 8])][:n_tile]
    per_tile = half // (8 * SUB)
    n_unit = n_tile * per_tile
    me = lax.axis_index('data')
    core, my_x, my_y, my_z = me % 2, (me // 2) % 2, (me // 4) % 2, me // 8
    top_z = n_dev // 8 - 1
    x_dev, y_dev, pair_dev = me + 2 - 4 * my_x, me + 4 - 8 * my_y, me + 1 - 2 * core
    up_dev, dn_dev = me + 8, me - 8

    barrier = pltpu.get_barrier_semaphore()
    for dev in (x_dev, y_dev, pair_dev):
        pl.semaphore_signal(barrier, inc=1, device_id=(dev,), device_id_type=MESH_ID)

    z_devs = [me + 8 * ((my_z + dist) % (top_z + 1) - my_z) for dist in range(1, top_z + 1)]
    for dev in z_devs:
        pl.semaphore_signal(barrier, inc=1, device_id=(dev,), device_id_type=MESH_ID)
    pl.semaphore_wait(barrier, 3 + top_z)

    def remote(src, dst, send_sem, recv_sem, dev):
        return pltpu.make_async_remote_copy(src_ref=src, dst_ref=dst, send_sem=send_sem, recv_sem=recv_sem, device_id=(dev,), device_id_type=MESH_ID)

    def factor_copies(slot, source):
        lhs, left, rhs, right = source
        mine = pl.ds(pl.multiple_of(left + core * half, 128), half)
        other = pl.ds(pl.multiple_of(left + (1 - core) * half, 128), half)
        lo, hi = pl.ds(0, toks), pl.ds(toks, toks)
        cols = pl.ds(right, WIDTH)
        return (
            pltpu.make_async_copy(lhs.at[:, mine], fa.at[slot, lo], fl_a.at[slot]),
            pltpu.make_async_copy(rhs.at[:, cols], fb.at[slot, lo], fl_b.at[slot]),
            remote(lhs.at[:, other], fa.at[slot, hi], fs_a.at[slot], fr_a.at[slot], pair_dev),
            remote(rhs.at[:, cols], fb.at[slot, hi], fs_b.at[slot], fr_b.at[slot], pair_dev),
        )

    for tile in range(2):
        for copy in factor_copies(tile, tiles[tile]):
            copy.start()

    def stream_stages(s):
        my_a, my_b = (my_x, my_y) if s == 0 else (my_y, my_x)
        a_dev, b_dev = (x_dev, y_dev) if s == 0 else (y_dev, x_dev)

        def root_of(u):
            return (u + 2 * s) % (top_z + 1)

        def part_rows(u, side):
            return pl.ds(pl.multiple_of((u % per_tile) * (8 * SUB) + s * (4 * SUB) + side * (2 * SUB), 8), 2 * SUB)

        def part_at(u, side):
            return part.at[(u // per_tile) % 2, part_rows(u, side)]

        def out_at(u, which, side, b_side=None):
            base = (u // per_tile) * WIDTH + which * half + (u % per_tile) * (8 * SUB) + s * (4 * SUB) + side * (2 * SUB)
            if b_side is None:
                return g_ref.at[pl.ds(pl.multiple_of(base, 8), 2 * SUB)]
            return g_ref.at[pl.ds(pl.multiple_of(base + b_side * SUB, 8), SUB)]

        def a_copy(u):
            k = u % RING
            return remote(part_at(u, 1 - my_a), ra.at[s, k], ra_s.at[s, k], ra_r.at[s, k], a_dev)

        def up_copy(u):
            k = u % RING
            return remote(acc.at[s, k], rzb.at[s, k], z_s.at[s, k], zb_r.at[s, k], up_dev)

        def dn_copy(u):
            k = u % RING
            return remote(acc.at[s, k], rza.at[s, k], z_s.at[s, k], za_r.at[s, k], dn_dev)

        def b_rows(side):
            return pl.ds(pl.multiple_of(side * SUB, 8), SUB)

        def b_copy(u):
            k = u % RING
            return remote(acc.at[s, k, b_rows(1 - my_b)], rb.at[s, k], b_s.at[s, k], b_r.at[s, k], b_dev)

        def bag_copy(u, b_side):
            k = u % RING
            return remote(fin.at[s, k], out_at(u, core, my_a, b_side), bag_s.at[s, k], bag_r.at[s, k], b_dev)

        def loc_copy(u):
            k = u % RING
            return pltpu.make_async_copy(fin.at[s, k], out_at(u, core, my_a, my_b), loc.at[s, k])

        def cast_up(u):
            k = u % RING
            rows = out_at(u, core, my_a)
            return remote(rows, rows, up_s.at[s, k], bc_r.at[s, k], up_dev)

        def cast_dn(u):
            k = u % RING
            rows = out_at(u, core, my_a)
            return remote(rows, rows, dn_s.at[s, k], bc_r.at[s, k], dn_dev)

        def aag_copy(u, side):
            k = u % RING
            rows = out_at(u, core, side)
            return remote(rows, rows, aag_s.at[s, k], aag_r.at[s, k], a_dev)

        def p1_copy(u, which):
            k = u % RING
            rows = out_at(u, which, my_a)
            return remote(rows, rows, p1_s.at[s, k], p1_r.at[s, k], pair_dev)

        def p2_copy(u, which):
            k = u % RING
            rows = out_at(u, which, 1 - my_a)
            return remote(rows, rows, p2_s.at[s, k], p2_r.at[s, k], pair_dev)

        def z_send(u, root):
            @pl.when(my_z < root)
            def _():
                up_copy(u).start()

            @pl.when(my_z > root)
            def _():
                dn_copy(u).start()

        def take_below(u):
            k = u % RING
            up_copy(u).wait_recv()
            acc[s, k] = acc[s, k] + rzb[s, k]

        def take_above(u):
            k = u % RING
            dn_copy(u).wait_recv()
            acc[s, k] = acc[s, k] + rza[s, k]

        def stage_first(u):
            a_copy(u).start()

        def stage_pair(u):
            k = u % RING
            root = root_of(u)
            a_copy(u).wait_recv()
            acc[s, k] = part[(u // per_tile) % 2, part_rows(u, my_a)] + ra[s, k]
            a_copy(u).wait_send()

            @pl.when((my_z == 0) | (my_z == top_z))
            def _():
                z_send(u, root)

        def stage_line(level, u):
            root = root_of(u)

            @pl.when((my_z < root) & (my_z == level))
            def _():
                take_below(u)
                up_copy(u).start()

            @pl.when((my_z > root) & (top_z - my_z == level))
            def _():
                take_above(u)
                dn_copy(u).start()

        def stage_root(u):
            @pl.when(my_z == root_of(u))
            def _():
                @pl.when(my_z > 0)
                def _():
                    take_below(u)

                @pl.when(my_z < top_z)
                def _():
                    take_above(u)

                b_copy(u).start()

        def stage_final(u):
            k = u % RING

            @pl.when(my_z == root_of(u))
            def _():
                b_copy(u).wait_recv()
                fin[s, k] = (acc[s, k, b_rows(my_b)] + rb[s, k]) * (1.0 / n_dev)
                bag_copy(u, my_b).start()
                loc_copy(u).start()
                b_copy(u).wait_send()

        def send_on(u, root):
            @pl.when((my_z >= root) & (my_z < top_z))
            def _():
                cast_up(u).start()

            @pl.when((my_z <= root) & (my_z > 0))
            def _():
                cast_dn(u).start()

            aag_copy(u, my_a).start()
            p1_copy(u, core).start()

        def stage_cast(dist, u):
            root = root_of(u)
            if dist == 0:
                @pl.when(my_z == root)
                def _():
                    loc_copy(u).wait()
                    bag_copy(u, my_b).wait_send()
                    bag_copy(u, 1 - my_b).wait_recv()
                    send_on(u, root)
            else:
                @pl.when((my_z == root + dist) | (my_z == root - dist))
                def _():
                    cast_up(u).wait_recv()
                    up_copy(u).wait_send()
                    send_on(u, root)

        def stage_swap(u):
            aag_copy(u, 1 - my_a).wait_recv()
            p2_copy(u, core).start()

        def stage_done(u):
            root = root_of(u)
            p1_copy(u, 1 - core).wait_recv()
            p2_copy(u, 1 - core).wait_recv()

            @pl.when((my_z >= root) & (my_z < top_z))
            def _():
                cast_up(u).wait_send()

            @pl.when((my_z <= root) & (my_z > 0))
            def _():
                cast_dn(u).wait_send()

            aag_copy(u, my_a).wait_send()
            p1_copy(u, core).wait_send()
            p2_copy(u, core).wait_send()

        stages = [stage_first, stage_pair]
        stages += [functools.partial(stage_line, level) for level in range(1, top_z)]
        stages += [stage_root, stage_final]
        stages += [functools.partial(stage_cast, dist) for dist in range(top_z + 1)]
        stages += [stage_swap, stage_done]
        return stages

    gain_devs = (pair_dev, x_dev, y_dev)

    def gain_copy(hop):
        return remote(gs.at[hop], gr.at[hop], gs_s.at[hop], gs_r.at[hop], gain_devs[hop])

    def gain_line(dist, slot):
        return remote(gs.at[3], gz.at[slot], gz_s.at[dist], gz_r.at[slot], z_devs[dist])

    def gain_steps(t):
        @pl.when(t == gain_start)
        def _():
            gain_copy(0).start()

        for hop in range(1, 4):
            @pl.when(t == gain_start + 4 * hop)
            def _():
                gain_copy(hop - 1).wait()
                gs[hop] = gs[hop - 1] + gr[hop - 1]
                if hop < 3:
                    gain_copy(hop).start()
                else:
                    gz[my_z] = gs[hop]
                    for dist in range(top_z):
                        gain_line(dist, my_z).start()

        @pl.when(t == gain_start + 16)
        def _():
            for dist in range(top_z):
                gain_line(dist, my_z).wait_send()
                gain_line(dist, (my_z + dist + 1) % (top_z + 1)).wait_recv()
            total = gz[0]
            for slot in range(1, top_z + 1):
                total = total + gz[slot]
            gain_out[...] = total * (1.0 / n_dev)

    streams = [stream_stages(0), stream_stages(1)]
    n_stage = len(streams[0])

    def step(t, carry):
        tile = t // per_tile
        gain_steps(t)

        for stage_idx in reversed(range(1, n_stage)):
            u = t - HOP * stage_idx

            @pl.when((u >= 0) & (u < n_unit))
            def _():
                for stages in streams:
                    stages[stage_idx](u)

        @pl.when((t < n_unit) & (t % per_tile == 0))
        def _():
            slot = tile % n_slot
            for copy in factor_copies(slot, tiles[0]):
                copy.wait()
            for lo in range(0, half, 128):
                part[tile % 2, lo:lo + 128, :] = lax.dot_general(
                    fa[slot, :, lo:lo + 128], fb[slot], (((0,), (0,)), ((), ())), preferred_element_type=jnp.float32)

            for later in range(2, n_tile):
                @pl.when(tile + 2 == later)
                def _():
                    for copy in factor_copies(later % n_slot, tiles[later]):
                        copy.start()

        @pl.when(t < n_unit)
        def _():
            for stages in streams:
                stages[0](t)

        piece(t)
        return carry

    gs[0] = gain_ref[...]
    prologue()
    lax.fori_loop(0, n_unit + HOP * (n_stage - 1), step, 0)


def reduce_tiles(top_factors, lower, saved, weights, gain_one, gain_two, gains, dx_top, n_tile, n_dev):
    n_layers = len(lower) + 1
    n_low = n_layers - 1
    toks = dx_top.shape[0]
    half = WIDTH // 2
    f32, bf16 = jnp.float32, jnp.bfloat16
    dma = pltpu.SemaphoreType.DMA
    slots = pltpu.VMEM((2, RING, 2 * SUB, WIDTH), f32)
    flops = n_tile * 2 * half * 2 * toks * WIDTH
    anyspace, vmem = pl.BlockSpec(memory_space=pl.ANY), pl.BlockSpec(memory_space=pltpu.VMEM)
    operands = list(top_factors) + [ref for group in lower for ref in group] + [ref for group in saved for ref in group] + list(weights)
    outs = [(((n_tile * WIDTH, WIDTH), f32), anyspace), ((gains.shape, f32), vmem), (((toks, WIDTH), bf16), anyspace),
            (((n_low, toks, 3 * WIDTH), bf16), anyspace), (((n_low, toks, WIDTH), bf16), anyspace), (((n_low, toks, 4 * WIDTH), bf16), anyspace),
            (((max(n_low - 1, 1), toks, WIDTH), bf16), anyspace)]
    vm_shapes = [(2, WIDTH, WIDTH), (2, WIDTH, WIDTH), (2, toks, WIDTH), (toks, WIDTH), (WIDTH, WIDTH), (toks, 3 * WIDTH), (WIDTH, 3 * WIDTH), (toks, WIDTH),
                 (toks, 4 * WIDTH), (toks, WIDTH), (toks, 3 * WIDTH), (toks, WIDTH), (toks, WIDTH)]
    return pl.pallas_call(
        functools.partial(reduce_kernel, n_layers, n_tile, n_dev),
        out_shape=tuple(jax.ShapeDtypeStruct(*shape) for shape, _ in outs),
        in_specs=[anyspace] * len(operands) + [vmem, vmem, vmem, anyspace],
        out_specs=tuple(spec for _, spec in outs),
        scratch_shapes=[pltpu.VMEM((4,) + gains.shape, f32)] + [pltpu.VMEM(shape, bf16) for shape in vm_shapes] + [
            pltpu.VMEM((toks, WIDTH), f32), dma((12,)), dma((7,)),
            pltpu.VMEM((3,) + gains.shape, f32),
            pltpu.VMEM((n_dev // 8,) + gains.shape, f32),
            dma((3,)), dma((3,)), dma((n_dev // 8 - 1,)), dma((n_dev // 8,)),
            pltpu.VMEM((4, 2 * toks, half), bf16),
            pltpu.VMEM((4, 2 * toks, WIDTH), bf16),
            pltpu.VMEM((2, half, WIDTH), f32),
            slots, slots, slots, slots,
            pltpu.VMEM((2, RING, SUB, WIDTH), f32),
            pltpu.VMEM((2, RING, SUB, WIDTH), f32),
        ] + [dma((4,))] * 6 + [dma((2, RING))] * 19,
        compiler_params=pltpu.CompilerParams(collective_id=0, has_side_effects=True, vmem_limit_bytes=62 * 1024 * 1024),
        cost_estimate=pl.CostEstimate(flops=flops, bytes_accessed=n_tile * WIDTH * WIDTH * 8, transcendentals=0),
        name='reduce_tiles',
    )(*operands, gain_one, gain_two, gains, dx_top)


def spread_kernel(n_layers, src_ref, qkv_ref, out_ref, up_ref, down_ref, buf, read_sem, write_sem):
    moves = []
    for layer in range(n_layers):
        for j in range(TILES):
            if j < 3:
                dst = qkv_ref.at[layer, :, pl.ds(j * WIDTH, WIDTH)]
            elif j < 4:
                dst = out_ref.at[layer]
            elif j < 8:
                dst = up_ref.at[layer, :, pl.ds((j - 4) * WIDTH, WIDTH)]
            else:
                dst = down_ref.at[layer, pl.ds((j - 8) * WIDTH, WIDTH)]
            slot = len(moves) % SPREAD
            moves.append((pltpu.make_async_copy(src_ref.at[pl.ds(((n_layers - 1 - layer) * TILES + j) * WIDTH, WIDTH)], buf.at[slot], read_sem.at[slot]),
                          pltpu.make_async_copy(buf.at[slot], dst, write_sem.at[slot])))
    ahead = SPREAD // 2
    for read, _ in moves[:ahead]:
        read.start()
    for idx, (read, write) in enumerate(moves):
        if idx >= ahead:
            moves[idx - ahead][1].wait()
        if idx + ahead < len(moves):
            moves[idx + ahead][0].start()
        read.wait()
        write.start()
    for _, write in moves[-ahead:]:
        write.wait()


def spread_tiles(tiles, n_layers):
    f32 = jnp.float32
    anyspace = pl.BlockSpec(memory_space=pl.ANY)
    shapes = ((WIDTH, 3 * WIDTH), (WIDTH, WIDTH), (WIDTH, 4 * WIDTH), (4 * WIDTH, WIDTH))
    return pl.pallas_call(
        functools.partial(spread_kernel, n_layers),
        out_shape=tuple(jax.ShapeDtypeStruct((n_layers,) + shape, f32) for shape in shapes),
        in_specs=[anyspace],
        out_specs=(anyspace,) * 4,
        scratch_shapes=[pltpu.VMEM((SPREAD, WIDTH, WIDTH), f32), pltpu.SemaphoreType.DMA((SPREAD,)), pltpu.SemaphoreType.DMA((SPREAD,))],
        compiler_params=pltpu.CompilerParams(vmem_limit_bytes=32 * 1024 * 1024),
        name='spread_tiles',
    )(tiles)


def solution(mesh):
    n_dev = mesh.shape['data']

    def local_step(x_loc, grad_y_loc, gain_one, gain_two, w_qkv, w_out, w_up, w_down):
        n_layers = w_qkv.shape[0]
        hidden_x = x_loc[0]
        lower, saved = [], []
        for layer_idx in range(n_layers):
            hidden, act_lo, saved_vals, sent, kept = block_forward(hidden_x, gain_one[layer_idx], gain_two[layer_idx], w_qkv[layer_idx], w_out[layer_idx], w_up[layer_idx])
            if layer_idx + 1 < n_layers:
                lower.insert(0, sent)
                saved.insert(0, kept)
                hidden_x = hidden + mix_lo('sf,fd->sd', act_lo, w_down[layer_idx])
        top = n_layers - 1
        dx_top, top_one, top_two, factors = block_backward(grad_y_loc[0], saved_vals, w_qkv[top], w_out[top], w_up[top], w_down[top])
        zero = jnp.zeros_like(top_one)
        gains = jnp.stack([zero] * top + [top_one] + [zero] * top + [top_two] + [zero] * (-2 * n_layers % 8))
        tiles, gain_sum, grad_x = reduce_tiles(factors, lower, saved, (w_qkv, w_out, w_up, w_down), gain_one, gain_two, gains, dx_top, n_layers * TILES, n_dev)[:3]
        return (grad_x[None], gain_sum[:n_layers], gain_sum[n_layers:2 * n_layers]) + tuple(spread_tiles(tiles, n_layers))

    batch_spec = P('data')
    full_spec = P()
    return jax.shard_map(local_step, mesh=mesh, in_specs=(batch_spec, batch_spec) + (full_spec,) * 6, out_specs=(batch_spec,) + (full_spec,) * 6, check_vma=False)
```

```python
import functools
import math

import jax
import jax.numpy as jnp
from jax import lax
from jax.experimental import pallas as pl
from jax.experimental.pallas import tpu as pltpu
from jax.sharding import PartitionSpec as P

NORM_EPS = 1e-6
HEAD_DIM = 64
WIDTH = 768
TILES = 12
SUB = 8
RING = 24
SPREAD = 8
PIECES = 12
HOP = 3
MESH_ID = pl.DeviceIdType.MESH


def rms_gain(rows_f, gain_vec):
    return rows_f * lax.rsqrt(jnp.mean(rows_f * rows_f, axis=-1, keepdims=True) + NORM_EPS) * gain_vec


def gelu_tanh(pre_act):
    return jax.nn.gelu(pre_act, approximate=True)


def mix_lo(einsum_spec, lhs_arr, rhs_arr):
    return jnp.einsum(einsum_spec, lhs_arr, rhs_arr, preferred_element_type=jnp.float32).astype(jnp.bfloat16)


def dot_nt(lhs, rhs):
    return lax.dot_general(lhs, rhs, (((1,), (1,)), ((), ())), preferred_element_type=jnp.float32)


def dot_tn(lhs, rhs):
    return lax.dot_general(lhs, rhs, (((0,), (0,)), ((), ())), preferred_element_type=jnp.float32)


def head_probs(q_part, k_pair):
    scores = dot_nt(q_part, k_pair) * HEAD_DIM ** -0.5
    rows = lax.broadcasted_iota(jnp.int32, scores.shape, 0)
    cols = lax.broadcasted_iota(jnp.int32, scores.shape, 1)
    scores = jnp.where(rows >= cols, scores, -1e30)
    weights = jnp.exp(scores - jnp.max(scores, axis=-1, keepdims=True))
    return weights * (1.0 / jnp.sum(weights, axis=-1, keepdims=True))


def pair_masks(shape):
    first = lax.broadcasted_iota(jnp.int32, shape, 1) < HEAD_DIM
    return first, [jnp.where(first, 1.0, 0.0).astype(jnp.bfloat16), jnp.where(first, 0.0, 1.0).astype(jnp.bfloat16)]


def attn_fwd_kernel(q_ref, k_ref, v_ref, o_ref):
    q_pair, k_pair, v_pair = q_ref[...], k_ref[...], v_ref[...]
    first, masks = pair_masks(q_pair.shape)
    outs = [jnp.dot(head_probs(q_pair * mask, k_pair).astype(jnp.bfloat16), v_pair, preferred_element_type=jnp.float32) for mask in masks]
    o_ref[...] = jnp.where(first, outs[0], outs[1]).astype(jnp.bfloat16)


def pair_grads(q_pair, k_pair, v_pair, do_pair):
    first, masks = pair_masks(q_pair.shape)
    grads = []
    for mask in masks:
        prob = head_probs(q_pair * mask, k_pair)
        grad_prob = dot_nt(do_pair * mask, v_pair)
        grad_score = (prob * (grad_prob - jnp.sum(prob * grad_prob, axis=-1, keepdims=True)) * HEAD_DIM ** -0.5).astype(jnp.bfloat16)
        grads.append((
            jnp.dot(grad_score, k_pair, preferred_element_type=jnp.float32),
            dot_tn(grad_score, q_pair),
            dot_tn(prob.astype(jnp.bfloat16), do_pair),
        ))
    return [jnp.where(first, grads[0][idx], grads[1][idx]).astype(jnp.bfloat16) for idx in range(3)]


def attn_specs(rows, count):
    pairs = WIDTH // (2 * HEAD_DIM)
    return pairs, [pl.BlockSpec((rows, 2 * HEAD_DIM), lambda h, lo=lo * pairs: (0, lo + h)) for lo in range(count)]


def attention(qkv):
    rows = qkv.shape[0]
    pairs, specs = attn_specs(rows, 3)
    return pl.pallas_call(
        attn_fwd_kernel, grid=(pairs,), in_specs=specs, out_specs=attn_specs(rows, 1)[1][0],
        out_shape=jax.ShapeDtypeStruct((rows, WIDTH), jnp.bfloat16), name='attn_fwd',
    )(qkv, qkv, qkv)


def block_forward(x_blk, gain_a, gain_b, w_qkv, w_out, w_up):
    u_one = rms_gain(x_blk.astype(jnp.float32), gain_a).astype(jnp.bfloat16)
    qkv_lo = mix_lo('sd,de->se', u_one, w_qkv)
    attn_out = attention(qkv_lo)
    hidden = x_blk + mix_lo('sd,de->se', attn_out, w_out)
    u_two = rms_gain(hidden.astype(jnp.float32), gain_b).astype(jnp.bfloat16)
    pre_lo = mix_lo('sd,df->sf', u_two, w_up)
    act_lo = gelu_tanh(pre_lo.astype(jnp.float32)).astype(jnp.bfloat16)
    return hidden, act_lo, (u_one, attn_out, u_two, act_lo), (x_blk, hidden, pre_lo, qkv_lo)


def layer_tiles(factors):
    u_one, grad_qkv, attn_out, grad_hidden, u_two, grad_pre, act_lo, grad_blk = factors
    tiles = []
    for lhs, rhs in ((act_lo, grad_blk), (u_two, grad_pre), (attn_out, grad_hidden), (u_one, grad_qkv)):
        tiles += [(lhs, left, rhs, right) for left in range(0, lhs.shape[1], WIDTH) for right in range(0, rhs.shape[1], WIDTH)]
    return tiles


def norm_grad(rows, gain, grad_out):
    scale = lax.rsqrt(jnp.mean(rows * rows, axis=-1, keepdims=True) + NORM_EPS)
    grad_gain = jnp.sum(grad_out * rows * scale, axis=0, keepdims=True)
    grad_unit = grad_out * gain
    grad_rows = grad_unit * scale - rows * (scale * scale * scale) * jnp.mean(rows * grad_unit, axis=-1, keepdims=True)
    return grad_rows, grad_gain


def gelu_slope(z):
    const = (2.0 / math.pi) ** 0.5
    curve = jnp.tanh(const * (z + 0.044715 * (z * z * z)))
    return 0.5 * (1.0 + curve) + 0.5 * z * (1.0 - curve * curve) * const * (1.0 + 3.0 * 0.044715 * (z * z))


def backward_pieces(n_layers, stride, saved, weights, gain_one, gain_two, grads_hbm, dx_hbm, grad_x, gs, vm, load, store):
    w_qkv, w_out, w_up, w_down = weights
    dqkv_hbm, dh_hbm, dz_hbm = grads_hbm
    w2, w1, zb, hb, wo, qkvb, wq, xb, dz, dh, dqkv, dy, do, acc = vm
    n_low = n_layers

    def cols(j):
        return pl.ds(pl.multiple_of(j * WIDTH, WIDTH), WIDTH)

    def weight_loads(low, j):
        layer, slot = n_layers - 1 - low, j % 2
        return (pltpu.make_async_copy(w_down.at[layer, cols(j)], w2.at[slot], load.at[slot]),
                pltpu.make_async_copy(w_up.at[layer, :, cols(j)], w1.at[slot], load.at[2 + slot]))

    def saved_load(kind, low, src_cols, dst, sem, act):
        for which in range(n_low):
            src = saved[which][kind] if src_cols is None else saved[which][kind].at[:, src_cols]

            @pl.when(low == which)
            def _():
                getattr(pltpu.make_async_copy(src, dst, sem), act)()

    def mlp_loads(low, j, act):
        for copy in weight_loads(low, j):
            getattr(copy, act)()
        saved_load(2, low, cols(j), zb.at[j % 2], load.at[4 + j % 2], act)

    def attn_loads(low, act):
        getattr(pltpu.make_async_copy(w_out.at[n_layers - 1 - low], wo, load.at[6]), act)()
        saved_load(1, low, None, hb, load.at[7], act)

    def last_loads(low, act):
        getattr(pltpu.make_async_copy(w_qkv.at[n_layers - 1 - low], wq, load.at[9]), act)()
        saved_load(0, low, None, xb, load.at[10], act)

    def add_gain(row, value):
        rows = lax.broadcasted_iota(jnp.int32, gs.shape[1:], 0)
        gs[0] = gs[0] + jnp.where(rows == row, value, 0.0)

    def prologue():
        first = pltpu.make_async_copy(dx_hbm[0], dy, load.at[11])
        first.start()
        mlp_loads(jnp.int32(0), jnp.int32(0), 'start')
        first.wait()

    def dz_out(low, j):
        return pltpu.make_async_copy(dz.at[:, cols(j)], dz_hbm.at[low, :, cols(j)], store.at[j])

    def piece(t):
        count = (t - 1) // stride
        low, p = count // PIECES, count % PIECES
        layer = n_layers - 1 - low
        active = (t >= 1) & ((t - 1) % stride == 0) & (count < n_low * PIECES)

        @pl.when(active & (p < 4))
        def _():
            mlp_loads(low, p, 'wait')

            @pl.when(p < 3)
            def _():
                mlp_loads(low, p + 1, 'start')

            @pl.when(p == 3)
            def _():
                attn_loads(low, 'start')
                saved_load(3, low, None, qkvb, load.at[8], 'start')

            slot = p % 2
            grad_act = dot_nt(dy[...], w2[slot]).astype(jnp.bfloat16).astype(jnp.float32)
            grad_pre = (gelu_slope(zb[slot].astype(jnp.float32)) * grad_act).astype(jnp.bfloat16)
            dz[:, cols(p)] = grad_pre
            term = dot_nt(grad_pre, w1[slot])

            @pl.when(p == 0)
            def _():
                acc[...] = term

            @pl.when(p > 0)
            def _():
                acc[...] = acc[...] + term

            dz_out(low, p).start()

        @pl.when(active & (p == 4))
        def _():
            attn_loads(low, 'wait')
            last_loads(low, 'start')
            grad_out = acc[...].astype(jnp.bfloat16).astype(jnp.float32)
            gain = gain_two[pl.ds(layer, 1), :]
            grad_rows, grad_gain = norm_grad(hb[...].astype(jnp.float32), gain, grad_out)
            dh[...] = (dy[...].astype(jnp.float32) + grad_rows).astype(jnp.bfloat16)
            add_gain(n_layers + layer, grad_gain)
            do[...] = dot_nt(dh[...], wo[...]).astype(jnp.bfloat16)
            pltpu.make_async_copy(dh, dh_hbm.at[low], store.at[4]).start()
            saved_load(3, low, None, qkvb, load.at[8], 'wait')
            for j in range(4):
                dz_out(low, j).wait()

        @pl.when(active & (p >= 5) & (p < 11))
        def _():
            def pair_cols(part_idx):
                return pl.ds(pl.multiple_of(part_idx * WIDTH + (p - 5) * 2 * HEAD_DIM, 2 * HEAD_DIM), 2 * HEAD_DIM)

            pair = pair_grads(qkvb[:, pair_cols(0)], qkvb[:, pair_cols(1)], qkvb[:, pair_cols(2)], do[:, pair_cols(0)])
            for part_idx in range(3):
                dqkv[:, pair_cols(part_idx)] = pair[part_idx]

        @pl.when(active & (p == 11))
        def _():
            last_loads(low, 'wait')
            dqkv_out = pltpu.make_async_copy(dqkv, dqkv_hbm.at[low], store.at[5])
            dqkv_out.start()

            @pl.when(low + 1 < n_low)
            def _():
                mlp_loads(low + 1, jnp.int32(0), 'start')

            grad_out = dot_nt(dqkv[...], wq[...]).astype(jnp.bfloat16).astype(jnp.float32)
            gain = gain_one[pl.ds(layer, 1), :]
            grad_rows, grad_gain = norm_grad(xb[...].astype(jnp.float32), gain, grad_out)
            add_gain(layer, grad_gain)
            dy[...] = (dh[...].astype(jnp.float32) + grad_rows).astype(jnp.bfloat16)
            for which in range(n_low):
                dst = grad_x if which == n_low - 1 else dx_hbm[which + 1]

                @pl.when(low == which)
                def _():
                    out = pltpu.make_async_copy(dy, dst, store.at[6])
                    out.start()
                    out.wait()

            pltpu.make_async_copy(dh, dh_hbm.at[low], store.at[4]).wait()
            dqkv_out.wait()

    return prologue, piece


def reduce_kernel(n_layers, n_tile, n_dev, *refs):
    refs = list(refs)

    def take(count):
        out = refs[:count]
        del refs[:count]
        return out

    lower = [take(4) for _ in range(n_layers)]
    saved = [take(4) for _ in range(n_layers)]
    weights = take(4)
    gain_one, gain_two, dx_top = take(3)
    g_ref, gain_out, grad_x, dqkv_hbm, dh_hbm, dz_hbm, dx_mid = take(7)
    dx_hbm = [dx_top] + [dx_mid.at[which] for which in range(n_layers - 1)]
    gs, *vm = take(15)
    load, store = take(2)
    stride = WIDTH // (16 * SUB) // 3
    prologue, piece = backward_pieces(n_layers, stride, saved, weights, gain_one, gain_two, (dqkv_hbm, dh_hbm, dz_hbm), dx_hbm, grad_x, gs, vm, load, store)
    f_refs = []
    for low in range(n_layers):
        u_one, attn_out, u_two, act_lo = lower[low]
        f_refs += [u_one, dqkv_hbm.at[low], attn_out, dh_hbm.at[low], u_two, dz_hbm.at[low], act_lo, dx_hbm[low]]
    reduce_body(n_tile, n_dev, prologue, piece, n_layers * PIECES * stride + 2, f_refs, g_ref, gain_out, gs, *refs)


def reduce_body(n_tile, n_dev, prologue, piece, gain_start, f_refs, g_ref, gain_out, gs, gr, gz, gs_s, gs_r, gz_s, gz_r, fa, fb, part, ra, acc, rzb, rza, rb, fin,
                fl_a, fl_b, fs_a, fs_b, fr_a, fr_b,
                ra_s, ra_r, z_s, zb_r, za_r, b_s, b_r, bag_s, bag_r, loc, bc_r, up_s, dn_s, aag_s, aag_r, p1_s, p1_r, p2_s, p2_r):
    toks = f_refs[0].shape[0]
    half = WIDTH // 2
    n_slot = fa.shape[0]
    tiles = [tile for lo in range(0, len(f_refs), 8) for tile in layer_tiles(f_refs[lo:lo + 8])][:n_tile]
    per_tile = half // (8 * SUB)
    n_unit = n_tile * per_tile
    me = lax.axis_index('data')
    core, my_x, my_y, my_z = me % 2, (me // 2) % 2, (me // 4) % 2, me // 8
    top_z = n_dev // 8 - 1
    x_dev, y_dev, pair_dev = me + 2 - 4 * my_x, me + 4 - 8 * my_y, me + 1 - 2 * core
    up_dev, dn_dev = me + 8, me - 8

    barrier = pltpu.get_barrier_semaphore()
    for dev in (x_dev, y_dev, pair_dev):
        pl.semaphore_signal(barrier, inc=1, device_id=(dev,), device_id_type=MESH_ID)

    z_devs = [me + 8 * ((my_z + dist) % (top_z + 1) - my_z) for dist in range(1, top_z + 1)]
    for dev in z_devs:
        pl.semaphore_signal(barrier, inc=1, device_id=(dev,), device_id_type=MESH_ID)
    pl.semaphore_wait(barrier, 3 + top_z)

    def remote(src, dst, send_sem, recv_sem, dev):
        return pltpu.make_async_remote_copy(src_ref=src, dst_ref=dst, send_sem=send_sem, recv_sem=recv_sem, device_id=(dev,), device_id_type=MESH_ID)

    def factor_copies(slot, source):
        lhs, left, rhs, right = source
        mine = pl.ds(pl.multiple_of(left + core * half, 128), half)
        other = pl.ds(pl.multiple_of(left + (1 - core) * half, 128), half)
        lo, hi = pl.ds(0, toks), pl.ds(toks, toks)
        cols = pl.ds(right, WIDTH)
        return (
            pltpu.make_async_copy(lhs.at[:, mine], fa.at[slot, lo], fl_a.at[slot]),
            pltpu.make_async_copy(rhs.at[:, cols], fb.at[slot, lo], fl_b.at[slot]),
            remote(lhs.at[:, other], fa.at[slot, hi], fs_a.at[slot], fr_a.at[slot], pair_dev),
            remote(rhs.at[:, cols], fb.at[slot, hi], fs_b.at[slot], fr_b.at[slot], pair_dev),
        )

    for tile in range(2):
        for copy in factor_copies(tile, tiles[tile]):
            copy.start()

    def stream_stages(s):
        my_a, my_b = (my_x, my_y) if s == 0 else (my_y, my_x)
        a_dev, b_dev = (x_dev, y_dev) if s == 0 else (y_dev, x_dev)

        def root_of(u):
            return (u + 2 * s) % (top_z + 1)

        def part_rows(u, side):
            return pl.ds(pl.multiple_of((u % per_tile) * (8 * SUB) + s * (4 * SUB) + side * (2 * SUB), 8), 2 * SUB)

        def part_at(u, side):
            return part.at[(u // per_tile) % 2, part_rows(u, side)]

        def out_at(u, which, side, b_side=None):
            base = (u // per_tile) * WIDTH + which * half + (u % per_tile) * (8 * SUB) + s * (4 * SUB) + side * (2 * SUB)
            if b_side is None:
                return g_ref.at[pl.ds(pl.multiple_of(base, 8), 2 * SUB)]
            return g_ref.at[pl.ds(pl.multiple_of(base + b_side * SUB, 8), SUB)]

        def a_copy(u):
            k = u % RING
            return remote(part_at(u, 1 - my_a), ra.at[s, k], ra_s.at[s, k], ra_r.at[s, k], a_dev)

        def up_copy(u):
            k = u % RING
            return remote(acc.at[s, k], rzb.at[s, k], z_s.at[s, k], zb_r.at[s, k], up_dev)

        def dn_copy(u):
            k = u % RING
            return remote(acc.at[s, k], rza.at[s, k], z_s.at[s, k], za_r.at[s, k], dn_dev)

        def b_rows(side):
            return pl.ds(pl.multiple_of(side * SUB, 8), SUB)

        def b_copy(u):
            k = u % RING
            return remote(acc.at[s, k, b_rows(1 - my_b)], rb.at[s, k], b_s.at[s, k], b_r.at[s, k], b_dev)

        def bag_copy(u, b_side):
            k = u % RING
            return remote(fin.at[s, k], out_at(u, core, my_a, b_side), bag_s.at[s, k], bag_r.at[s, k], b_dev)

        def loc_copy(u):
            k = u % RING
            return pltpu.make_async_copy(fin.at[s, k], out_at(u, core, my_a, my_b), loc.at[s, k])

        def cast_up(u):
            k = u % RING
            rows = out_at(u, core, my_a)
            return remote(rows, rows, up_s.at[s, k], bc_r.at[s, k], up_dev)

        def cast_dn(u):
            k = u % RING
            rows = out_at(u, core, my_a)
            return remote(rows, rows, dn_s.at[s, k], bc_r.at[s, k], dn_dev)

        def aag_copy(u, side):
            k = u % RING
            rows = out_at(u, core, side)
            return remote(rows, rows, aag_s.at[s, k], aag_r.at[s, k], a_dev)

        def p1_copy(u, which):
            k = u % RING
            rows = out_at(u, which, my_a)
            return remote(rows, rows, p1_s.at[s, k], p1_r.at[s, k], pair_dev)

        def p2_copy(u, which):
            k = u % RING
            rows = out_at(u, which, 1 - my_a)
            return remote(rows, rows, p2_s.at[s, k], p2_r.at[s, k], pair_dev)

        def z_send(u, root):
            @pl.when(my_z < root)
            def _():
                up_copy(u).start()

            @pl.when(my_z > root)
            def _():
                dn_copy(u).start()

        def take_below(u):
            k = u % RING
            up_copy(u).wait_recv()
            acc[s, k] = acc[s, k] + rzb[s, k]

        def take_above(u):
            k = u % RING
            dn_copy(u).wait_recv()
            acc[s, k] = acc[s, k] + rza[s, k]

        def stage_first(u):
            a_copy(u).start()

        def stage_pair(u):
            k = u % RING
            root = root_of(u)
            a_copy(u).wait_recv()
            acc[s, k] = part[(u // per_tile) % 2, part_rows(u, my_a)] + ra[s, k]
            a_copy(u).wait_send()

            @pl.when((my_z == 0) | (my_z == top_z))
            def _():
                z_send(u, root)

        def stage_line(level, u):
            root = root_of(u)

            @pl.when((my_z < root) & (my_z == level))
            def _():
                take_below(u)
                up_copy(u).start()

            @pl.when((my_z > root) & (top_z - my_z == level))
            def _():
                take_above(u)
                dn_copy(u).start()

        def stage_root(u):
            @pl.when(my_z == root_of(u))
            def _():
                @pl.when(my_z > 0)
                def _():
                    take_below(u)

                @pl.when(my_z < top_z)
                def _():
                    take_above(u)

                b_copy(u).start()

        def stage_final(u):
            k = u % RING

            @pl.when(my_z == root_of(u))
            def _():
                b_copy(u).wait_recv()
                fin[s, k] = (acc[s, k, b_rows(my_b)] + rb[s, k]) * (1.0 / n_dev)
                bag_copy(u, my_b).start()
                loc_copy(u).start()
                b_copy(u).wait_send()

        def send_on(u, root):
            @pl.when((my_z >= root) & (my_z < top_z))
            def _():
                cast_up(u).start()

            @pl.when((my_z <= root) & (my_z > 0))
            def _():
                cast_dn(u).start()

            aag_copy(u, my_a).start()
            p1_copy(u, core).start()

        def stage_cast(dist, u):
            root = root_of(u)
            if dist == 0:
                @pl.when(my_z == root)
                def _():
                    loc_copy(u).wait()
                    bag_copy(u, my_b).wait_send()
                    bag_copy(u, 1 - my_b).wait_recv()
                    send_on(u, root)
            else:
                @pl.when((my_z == root + dist) | (my_z == root - dist))
                def _():
                    cast_up(u).wait_recv()
                    up_copy(u).wait_send()
                    send_on(u, root)

        def stage_swap(u):
            aag_copy(u, 1 - my_a).wait_recv()
            p2_copy(u, core).start()

        def stage_done(u):
            root = root_of(u)
            p1_copy(u, 1 - core).wait_recv()
            p2_copy(u, 1 - core).wait_recv()

            @pl.when((my_z >= root) & (my_z < top_z))
            def _():
                cast_up(u).wait_send()

            @pl.when((my_z <= root) & (my_z > 0))
            def _():
                cast_dn(u).wait_send()

            aag_copy(u, my_a).wait_send()
            p1_copy(u, core).wait_send()
            p2_copy(u, core).wait_send()

        stages = [stage_first, stage_pair]
        stages += [functools.partial(stage_line, level) for level in range(1, top_z)]
        stages += [stage_root, stage_final]
        stages += [functools.partial(stage_cast, dist) for dist in range(top_z + 1)]
        stages += [stage_swap, stage_done]
        return stages

    gain_devs = (pair_dev, x_dev, y_dev)

    def gain_copy(hop):
        return remote(gs.at[hop], gr.at[hop], gs_s.at[hop], gs_r.at[hop], gain_devs[hop])

    def gain_line(dist, slot):
        return remote(gs.at[3], gz.at[slot], gz_s.at[dist], gz_r.at[slot], z_devs[dist])

    def gain_steps(t):
        @pl.when(t == gain_start)
        def _():
            gain_copy(0).start()

        for hop in range(1, 4):
            @pl.when(t == gain_start + 4 * hop)
            def _():
                gain_copy(hop - 1).wait()
                gs[hop] = gs[hop - 1] + gr[hop - 1]
                if hop < 3:
                    gain_copy(hop).start()
                else:
                    gz[my_z] = gs[hop]
                    for dist in range(top_z):
                        gain_line(dist, my_z).start()

        @pl.when(t == gain_start + 16)
        def _():
            for dist in range(top_z):
                gain_line(dist, my_z).wait_send()
                gain_line(dist, (my_z + dist + 1) % (top_z + 1)).wait_recv()
            total = gz[0]
            for slot in range(1, top_z + 1):
                total = total + gz[slot]
            gain_out[...] = total * (1.0 / n_dev)

    streams = [stream_stages(0), stream_stages(1)]
    n_stage = len(streams[0])

    def step(t, carry):
        tile = t // per_tile
        gain_steps(t)

        for stage_idx in reversed(range(1, n_stage)):
            u = t - HOP * stage_idx

            @pl.when((u >= 0) & (u < n_unit))
            def _():
                for stages in streams:
                    stages[stage_idx](u)

        @pl.when((t < n_unit) & (t % per_tile == 0))
        def _():
            slot = tile % n_slot
            for copy in factor_copies(slot, tiles[0]):
                copy.wait()
            for lo in range(0, half, 128):
                part[tile % 2, lo:lo + 128, :] = lax.dot_general(
                    fa[slot, :, lo:lo + 128], fb[slot], (((0,), (0,)), ((), ())), preferred_element_type=jnp.float32)

            for later in range(2, n_tile):
                @pl.when(tile + 2 == later)
                def _():
                    for copy in factor_copies(later % n_slot, tiles[later]):
                        copy.start()

        @pl.when(t < n_unit)
        def _():
            for stages in streams:
                stages[0](t)

        piece(t)
        return carry

    gs[0] = jnp.zeros(gs.shape[1:], jnp.float32)
    prologue()
    lax.fori_loop(0, n_unit + HOP * (n_stage - 1), step, 0)


def reduce_tiles(lower, saved, weights, gain_one, gain_two, dx_top, n_tile, n_dev):
    n_layers = n_low = len(lower)
    gains = jax.ShapeDtypeStruct((-(-2 * n_layers // 8) * 8, WIDTH), jnp.float32)
    toks = dx_top.shape[0]
    half = WIDTH // 2
    f32, bf16 = jnp.float32, jnp.bfloat16
    dma = pltpu.SemaphoreType.DMA
    slots = pltpu.VMEM((2, RING, 2 * SUB, WIDTH), f32)
    flops = n_tile * 2 * half * 2 * toks * WIDTH
    anyspace, vmem = pl.BlockSpec(memory_space=pl.ANY), pl.BlockSpec(memory_space=pltpu.VMEM)
    operands = [ref for group in lower for ref in group] + [ref for group in saved for ref in group] + list(weights)
    outs = [(((n_tile * WIDTH, WIDTH), f32), anyspace), ((gains.shape, f32), vmem), (((toks, WIDTH), bf16), anyspace),
            (((n_low, toks, 3 * WIDTH), bf16), anyspace), (((n_low, toks, WIDTH), bf16), anyspace), (((n_low, toks, 4 * WIDTH), bf16), anyspace),
            (((n_layers - 1, toks, WIDTH), bf16), anyspace)]
    vm_shapes = [(2, WIDTH, WIDTH), (2, WIDTH, WIDTH), (2, toks, WIDTH), (toks, WIDTH), (WIDTH, WIDTH), (toks, 3 * WIDTH), (WIDTH, 3 * WIDTH), (toks, WIDTH),
                 (toks, 4 * WIDTH), (toks, WIDTH), (toks, 3 * WIDTH), (toks, WIDTH), (toks, WIDTH)]
    return pl.pallas_call(
        functools.partial(reduce_kernel, n_layers, n_tile, n_dev),
        out_shape=tuple(jax.ShapeDtypeStruct(*shape) for shape, _ in outs),
        in_specs=[anyspace] * len(operands) + [vmem, vmem, anyspace],
        out_specs=tuple(spec for _, spec in outs),
        scratch_shapes=[pltpu.VMEM((4,) + gains.shape, f32)] + [pltpu.VMEM(shape, bf16) for shape in vm_shapes] + [
            pltpu.VMEM((toks, WIDTH), f32), dma((12,)), dma((7,)),
            pltpu.VMEM((3,) + gains.shape, f32),
            pltpu.VMEM((n_dev // 8,) + gains.shape, f32),
            dma((3,)), dma((3,)), dma((n_dev // 8 - 1,)), dma((n_dev // 8,)),
            pltpu.VMEM((4, 2 * toks, half), bf16),
            pltpu.VMEM((4, 2 * toks, WIDTH), bf16),
            pltpu.VMEM((2, half, WIDTH), f32),
            slots, slots, slots, slots,
            pltpu.VMEM((2, RING, SUB, WIDTH), f32),
            pltpu.VMEM((2, RING, SUB, WIDTH), f32),
        ] + [dma((4,))] * 6 + [dma((2, RING))] * 19,
        compiler_params=pltpu.CompilerParams(collective_id=0, has_side_effects=True, vmem_limit_bytes=62 * 1024 * 1024),
        cost_estimate=pl.CostEstimate(flops=flops, bytes_accessed=n_tile * WIDTH * WIDTH * 8, transcendentals=0),
        name='reduce_tiles',
    )(*operands, gain_one, gain_two, dx_top)


def spread_kernel(n_layers, src_ref, qkv_ref, out_ref, up_ref, down_ref, buf, read_sem, write_sem):
    moves = []
    for layer in range(n_layers):
        for j in range(TILES):
            if j < 4:
                dst = down_ref.at[layer, pl.ds(j * WIDTH, WIDTH)]
            elif j < 8:
                dst = up_ref.at[layer, :, pl.ds((j - 4) * WIDTH, WIDTH)]
            elif j < 9:
                dst = out_ref.at[layer]
            else:
                dst = qkv_ref.at[layer, :, pl.ds((j - 9) * WIDTH, WIDTH)]
            slot = len(moves) % SPREAD
            moves.append((pltpu.make_async_copy(src_ref.at[pl.ds(((n_layers - 1 - layer) * TILES + j) * WIDTH, WIDTH)], buf.at[slot], read_sem.at[slot]),
                          pltpu.make_async_copy(buf.at[slot], dst, write_sem.at[slot])))
    ahead = SPREAD // 2
    for read, _ in moves[:ahead]:
        read.start()
    for idx, (read, write) in enumerate(moves):
        if idx >= ahead:
            moves[idx - ahead][1].wait()
        if idx + ahead < len(moves):
            moves[idx + ahead][0].start()
        read.wait()
        write.start()
    for _, write in moves[-ahead:]:
        write.wait()


def spread_tiles(tiles, n_layers):
    f32 = jnp.float32
    anyspace = pl.BlockSpec(memory_space=pl.ANY)
    shapes = ((WIDTH, 3 * WIDTH), (WIDTH, WIDTH), (WIDTH, 4 * WIDTH), (4 * WIDTH, WIDTH))
    return pl.pallas_call(
        functools.partial(spread_kernel, n_layers),
        out_shape=tuple(jax.ShapeDtypeStruct((n_layers,) + shape, f32) for shape in shapes),
        in_specs=[anyspace],
        out_specs=(anyspace,) * 4,
        scratch_shapes=[pltpu.VMEM((SPREAD, WIDTH, WIDTH), f32), pltpu.SemaphoreType.DMA((SPREAD,)), pltpu.SemaphoreType.DMA((SPREAD,))],
        compiler_params=pltpu.CompilerParams(vmem_limit_bytes=32 * 1024 * 1024),
        name='spread_tiles',
    )(tiles)


def solution(mesh):
    n_dev = mesh.shape['data']

    def local_step(x_loc, grad_y_loc, gain_one, gain_two, w_qkv, w_out, w_up, w_down):
        n_layers = w_qkv.shape[0]
        hidden_x = x_loc[0]
        lower, saved = [], []
        for layer_idx in range(n_layers):
            hidden, act_lo, sent, kept = block_forward(hidden_x, gain_one[layer_idx], gain_two[layer_idx], w_qkv[layer_idx], w_out[layer_idx], w_up[layer_idx])
            lower.insert(0, sent)
            saved.insert(0, kept)
            if layer_idx + 1 < n_layers:
                hidden_x = hidden + mix_lo('sf,fd->sd', act_lo, w_down[layer_idx])
        tiles, gain_sum, grad_x = reduce_tiles(lower, saved, (w_qkv, w_out, w_up, w_down), gain_one, gain_two, grad_y_loc[0], n_layers * TILES, n_dev)[:3]
        return (grad_x[None], gain_sum[:n_layers], gain_sum[n_layers:2 * n_layers]) + tuple(spread_tiles(tiles, n_layers))

    batch_spec = P('data')
    full_spec = P()
    return jax.shard_map(local_step, mesh=mesh, in_specs=(batch_spec, batch_spec) + (full_spec,) * 6, out_specs=(batch_spec,) + (full_spec,) * 6, check_vma=False)
```

```python
import functools
import math

import jax
import jax.numpy as jnp
from jax import lax
from jax.experimental import pallas as pl
from jax.experimental.pallas import tpu as pltpu
from jax.sharding import PartitionSpec as P

NORM_EPS = 1e-6
HEAD_DIM = 64
WIDTH = 768
TILES = 12
SUB = 8
RING = 16
SPREAD = 8
PIECES = 12
HOP = 2
MESH_ID = pl.DeviceIdType.MESH


def rms_gain(rows_f, gain_vec):
    return rows_f * lax.rsqrt(jnp.mean(rows_f * rows_f, axis=-1, keepdims=True) + NORM_EPS) * gain_vec


def gelu_tanh(pre_act):
    return jax.nn.gelu(pre_act, approximate=True)


def dot_nt(lhs, rhs):
    return lax.dot_general(lhs, rhs, (((1,), (1,)), ((), ())), preferred_element_type=jnp.float32)


def dot_tn(lhs, rhs):
    return lax.dot_general(lhs, rhs, (((0,), (0,)), ((), ())), preferred_element_type=jnp.float32)


def head_probs(q_part, k_pair):
    scores = dot_nt(q_part, k_pair) * HEAD_DIM ** -0.5
    rows = lax.broadcasted_iota(jnp.int32, scores.shape, 0)
    cols = lax.broadcasted_iota(jnp.int32, scores.shape, 1)
    scores = jnp.where(rows >= cols, scores, -1e30)
    weights = jnp.exp(scores - jnp.max(scores, axis=-1, keepdims=True))
    return weights * (1.0 / jnp.sum(weights, axis=-1, keepdims=True))


def pair_masks(shape):
    first = lax.broadcasted_iota(jnp.int32, shape, 1) < HEAD_DIM
    return first, [jnp.where(first, 1.0, 0.0).astype(jnp.bfloat16), jnp.where(first, 0.0, 1.0).astype(jnp.bfloat16)]


def pair_grads(q_pair, k_pair, v_pair, do_pair):
    first, masks = pair_masks(q_pair.shape)
    grads = []
    for mask in masks:
        prob = head_probs(q_pair * mask, k_pair)
        grad_prob = dot_nt(do_pair * mask, v_pair)
        grad_score = (prob * (grad_prob - jnp.sum(prob * grad_prob, axis=-1, keepdims=True)) * HEAD_DIM ** -0.5).astype(jnp.bfloat16)
        grads.append((
            jnp.dot(grad_score, k_pair, preferred_element_type=jnp.float32),
            dot_tn(grad_score, q_pair),
            dot_tn(prob.astype(jnp.bfloat16), do_pair),
        ))
    return [jnp.where(first, grads[0][idx], grads[1][idx]).astype(jnp.bfloat16) for idx in range(3)]


def causal_rows(q_part, k_pair, v_pair, lo, count):
    keys = lo + count
    scores = dot_nt(q_part[lo:keys], k_pair[:keys]) * HEAD_DIM ** -0.5
    rows = lax.broadcasted_iota(jnp.int32, scores.shape, 0) + lo
    cols = lax.broadcasted_iota(jnp.int32, scores.shape, 1)
    scores = jnp.where(rows >= cols, scores, -1e30)
    weights = jnp.exp(scores - jnp.max(scores, axis=-1, keepdims=True))
    probs = (weights * (1.0 / jnp.sum(weights, axis=-1, keepdims=True))).astype(jnp.bfloat16)
    return jnp.dot(probs, v_pair[:keys], preferred_element_type=jnp.float32)


def forward_kernel(n_layers, x_ref, gain_one, gain_two, w_qkv, w_out, w_up, w_down,
                   x_all, u_one_all, qkv_all, attn_all, hidden_all, u_two_all, z_all, act_all,
                   wq, wo, w1, w2, x_v, u_one, qkv, attn, hidden, u_two, z_v, act, acc, load, store):
    f32, bf16 = jnp.float32, jnp.bfloat16
    toks = x_ref.shape[0]

    def loads(layer):
        slot = layer % 2
        return [pltpu.make_async_copy(src.at[layer], dst.at[slot], load.at[slot, idx])
                for idx, (src, dst) in enumerate(((w_qkv, wq), (w_out, wo), (w_up, w1), (w_down, w2)))]

    def saves(layer):
        pairs = ((x_v, x_all), (u_one, u_one_all), (qkv, qkv_all), (attn, attn_all), (hidden, hidden_all), (u_two, u_two_all), (z_v, z_all), (act, act_all))
        return [pltpu.make_async_copy(src, dst.at[layer], store.at[idx]) for idx, (src, dst) in enumerate(pairs)]

    for copy in loads(jnp.int32(0)):
        copy.start()
    x_v[...] = x_ref[...]

    def layer_step(layer, carry):
        slot = layer % 2
        weights, outs = loads(layer), saves(layer)

        def reuse(idx):
            @pl.when(layer > 0)
            def _():
                outs[idx].wait()

        @pl.when(layer + 1 < n_layers)
        def _():
            for copy in loads(layer + 1):
                copy.start()

        outs[0].start()
        reuse(1)
        u_one[...] = rms_gain(x_v[...].astype(f32), gain_one[pl.ds(layer, 1), :]).astype(bf16)
        outs[1].start()
        weights[0].wait()
        reuse(2)
        for j in range(3):
            cols = slice(j * WIDTH, (j + 1) * WIDTH)
            qkv[:, cols] = jnp.dot(u_one[...], wq[slot, :, cols], preferred_element_type=f32).astype(bf16)
        outs[2].start()
        reuse(3)

        def pair_step(pair, inner):
            def pair_cols(part_idx):
                return pl.ds(pl.multiple_of(part_idx * WIDTH + pair * 2 * HEAD_DIM, 2 * HEAD_DIM), 2 * HEAD_DIM)

            q_pair, k_pair, v_pair = (qkv[:, pair_cols(part_idx)] for part_idx in range(3))
            first, masks = pair_masks(q_pair.shape)
            heads = [q_pair * mask for mask in masks]
            for lo in range(0, toks, 128):
                out = [causal_rows(head, k_pair, v_pair, lo, 128) for head in heads]
                attn[lo:lo + 128, pair_cols(0)] = jnp.where(first[:128], out[0], out[1]).astype(bf16)
            return inner

        lax.fori_loop(0, WIDTH // (2 * HEAD_DIM), pair_step, 0)
        outs[3].start()
        weights[1].wait()
        mixed = jnp.dot(attn[...], wo[slot], preferred_element_type=f32).astype(bf16)
        reuse(4)
        hidden[...] = (x_v[...].astype(f32) + mixed.astype(f32)).astype(bf16)
        outs[4].start()
        reuse(5)
        u_two[...] = rms_gain(hidden[...].astype(f32), gain_two[pl.ds(layer, 1), :]).astype(bf16)
        outs[5].start()
        weights[2].wait()
        weights[3].wait()
        reuse(6)
        reuse(7)
        for j in range(4):
            cols = slice(j * WIDTH, (j + 1) * WIDTH)
            pre = jnp.dot(u_two[...], w1[slot, :, cols], preferred_element_type=f32).astype(bf16)
            z_v[:, cols] = pre
            act[:, cols] = gelu_tanh(pre.astype(f32)).astype(bf16)

            @pl.when(layer + 1 < n_layers)
            def _():
                term = jnp.dot(act[:, cols], w2[slot, cols], preferred_element_type=f32)
                acc[...] = term if j == 0 else acc[...] + term
        outs[6].start()
        outs[7].start()
        outs[0].wait()

        @pl.when(layer + 1 < n_layers)
        def _():
            x_v[...] = (hidden[...].astype(f32) + acc[...].astype(bf16).astype(f32)).astype(bf16)

        return carry

    lax.fori_loop(0, n_layers, layer_step, 0)
    for copy in saves(n_layers - 1)[1:]:
        copy.wait()


def forward(x_loc, gain_one, gain_two, weights):
    n_layers, toks = gain_one.shape[0], x_loc.shape[0]
    f32, bf16 = jnp.float32, jnp.bfloat16
    anyspace, vmem = pl.BlockSpec(memory_space=pl.ANY), pl.BlockSpec(memory_space=pltpu.VMEM)
    widths = (WIDTH, WIDTH, 3 * WIDTH, WIDTH, WIDTH, WIDTH, 4 * WIDTH, 4 * WIDTH)
    return pl.pallas_call(
        functools.partial(forward_kernel, n_layers),
        out_shape=tuple(jax.ShapeDtypeStruct((n_layers, toks, width), bf16) for width in widths),
        in_specs=[vmem, vmem, vmem] + [anyspace] * 4,
        out_specs=(anyspace,) * 8,
        scratch_shapes=[pltpu.VMEM((2,) + weight.shape[1:], bf16) for weight in weights] + [pltpu.VMEM((toks, width), bf16) for width in widths] + [
            pltpu.VMEM((toks, WIDTH), f32), pltpu.SemaphoreType.DMA((2, 4)), pltpu.SemaphoreType.DMA((8,))],
        compiler_params=pltpu.CompilerParams(vmem_limit_bytes=58 * 1024 * 1024),
        name='forward',
    )(x_loc, gain_one, gain_two, *weights)


def layer_tiles(factors):
    u_one, grad_qkv, attn_out, grad_hidden, u_two, grad_pre, act_lo, grad_blk = factors
    tiles = []
    for lhs, rhs in ((act_lo, grad_blk), (u_two, grad_pre), (attn_out, grad_hidden), (u_one, grad_qkv)):
        tiles += [(lhs, left, rhs, right) for left in range(0, lhs.shape[1], WIDTH) for right in range(0, rhs.shape[1], WIDTH)]
    return tiles


def norm_grad(rows, gain, grad_out):
    scale = lax.rsqrt(jnp.mean(rows * rows, axis=-1, keepdims=True) + NORM_EPS)
    grad_gain = jnp.sum(grad_out * rows * scale, axis=0, keepdims=True)
    grad_unit = grad_out * gain
    grad_rows = grad_unit * scale - rows * (scale * scale * scale) * jnp.mean(rows * grad_unit, axis=-1, keepdims=True)
    return grad_rows, grad_gain


def gelu_slope(z):
    const = (2.0 / math.pi) ** 0.5
    curve = jnp.tanh(const * (z + 0.044715 * (z * z * z)))
    return 0.5 * (1.0 + curve) + 0.5 * z * (1.0 - curve * curve) * const * (1.0 + 3.0 * 0.044715 * (z * z))


def backward_pieces(n_layers, stride, saved, weights, gain_one, gain_two, grads_hbm, dx_hbm, grad_x, gs, vm, load, store):
    w_qkv, w_out, w_up, w_down = weights
    dqkv_hbm, dh_hbm, dz_hbm = grads_hbm
    w2, w1, zb, hb, wo, qkvb, wq, xb, dz, dh, dqkv, dy, do, acc = vm
    n_low = n_layers

    def cols(j):
        return pl.ds(pl.multiple_of(j * WIDTH, WIDTH), WIDTH)

    def weight_loads(low, j):
        layer, slot = n_layers - 1 - low, j % 2
        return (pltpu.make_async_copy(w_down.at[layer, cols(j)], w2.at[slot], load.at[slot]),
                pltpu.make_async_copy(w_up.at[layer, :, cols(j)], w1.at[slot], load.at[2 + slot]))

    def saved_load(kind, low, src_cols, dst, sem, act):
        layer = n_layers - 1 - low
        src = saved[kind].at[layer] if src_cols is None else saved[kind].at[layer, :, src_cols]
        getattr(pltpu.make_async_copy(src, dst, sem), act)()

    def mlp_loads(low, j, act):
        for copy in weight_loads(low, j):
            getattr(copy, act)()
        saved_load(2, low, cols(j), zb.at[j % 2], load.at[4 + j % 2], act)

    def attn_loads(low, act):
        getattr(pltpu.make_async_copy(w_out.at[n_layers - 1 - low], wo, load.at[6]), act)()
        saved_load(1, low, None, hb, load.at[7], act)

    def last_loads(low, act):
        getattr(pltpu.make_async_copy(w_qkv.at[n_layers - 1 - low], wq, load.at[9]), act)()
        saved_load(0, low, None, xb, load.at[10], act)

    def add_gain(row, value):
        rows = lax.broadcasted_iota(jnp.int32, gs.shape[1:], 0)
        gs[0] = gs[0] + jnp.where(rows == row, value, 0.0)

    def prologue():
        first = pltpu.make_async_copy(dx_hbm[0], dy, load.at[11])
        first.start()
        mlp_loads(jnp.int32(0), jnp.int32(0), 'start')
        first.wait()

    def dz_out(low, j):
        return pltpu.make_async_copy(dz.at[:, cols(j)], dz_hbm.at[low, :, cols(j)], store.at[j])

    def piece(t):
        count = (t - 1) // stride
        low, p = count // PIECES, count % PIECES
        layer = n_layers - 1 - low
        active = (t >= 1) & ((t - 1) % stride == 0) & (count < n_low * PIECES)

        @pl.when(active & (p < 4))
        def _():
            mlp_loads(low, p, 'wait')

            @pl.when(p < 3)
            def _():
                mlp_loads(low, p + 1, 'start')

            @pl.when(p == 3)
            def _():
                attn_loads(low, 'start')
                saved_load(3, low, None, qkvb, load.at[8], 'start')

            slot = p % 2
            grad_act = dot_nt(dy[...], w2[slot]).astype(jnp.bfloat16).astype(jnp.float32)
            grad_pre = (gelu_slope(zb[slot].astype(jnp.float32)) * grad_act).astype(jnp.bfloat16)
            dz[:, cols(p)] = grad_pre
            term = dot_nt(grad_pre, w1[slot])

            @pl.when(p == 0)
            def _():
                acc[...] = term

            @pl.when(p > 0)
            def _():
                acc[...] = acc[...] + term

            dz_out(low, p).start()

        @pl.when(active & (p == 4))
        def _():
            attn_loads(low, 'wait')
            last_loads(low, 'start')
            grad_out = acc[...].astype(jnp.bfloat16).astype(jnp.float32)
            gain = gain_two[pl.ds(layer, 1), :]
            grad_rows, grad_gain = norm_grad(hb[...].astype(jnp.float32), gain, grad_out)
            dh[...] = (dy[...].astype(jnp.float32) + grad_rows).astype(jnp.bfloat16)
            add_gain(n_layers + layer, grad_gain)
            do[...] = dot_nt(dh[...], wo[...]).astype(jnp.bfloat16)
            pltpu.make_async_copy(dh, dh_hbm.at[low], store.at[4]).start()
            saved_load(3, low, None, qkvb, load.at[8], 'wait')
            for j in range(4):
                dz_out(low, j).wait()

        @pl.when(active & (p >= 5) & (p < 11))
        def _():
            def pair_cols(part_idx):
                return pl.ds(pl.multiple_of(part_idx * WIDTH + (p - 5) * 2 * HEAD_DIM, 2 * HEAD_DIM), 2 * HEAD_DIM)

            pair = pair_grads(qkvb[:, pair_cols(0)], qkvb[:, pair_cols(1)], qkvb[:, pair_cols(2)], do[:, pair_cols(0)])
            for part_idx in range(3):
                dqkv[:, pair_cols(part_idx)] = pair[part_idx]

        @pl.when(active & (p == 11))
        def _():
            last_loads(low, 'wait')
            dqkv_out = pltpu.make_async_copy(dqkv, dqkv_hbm.at[low], store.at[5])
            dqkv_out.start()

            @pl.when(low + 1 < n_low)
            def _():
                mlp_loads(low + 1, jnp.int32(0), 'start')

            grad_out = dot_nt(dqkv[...], wq[...]).astype(jnp.bfloat16).astype(jnp.float32)
            gain = gain_one[pl.ds(layer, 1), :]
            grad_rows, grad_gain = norm_grad(xb[...].astype(jnp.float32), gain, grad_out)
            add_gain(layer, grad_gain)
            dy[...] = (dh[...].astype(jnp.float32) + grad_rows).astype(jnp.bfloat16)
            for which in range(n_low):
                dst = grad_x if which == n_low - 1 else dx_hbm[which + 1]

                @pl.when(low == which)
                def _():
                    out = pltpu.make_async_copy(dy, dst, store.at[6])
                    out.start()
                    out.wait()

            pltpu.make_async_copy(dh, dh_hbm.at[low], store.at[4]).wait()
            dqkv_out.wait()

    return prologue, piece


def reduce_kernel(n_layers, n_tile, n_dev, *refs):
    refs = list(refs)

    def take(count):
        out = refs[:count]
        del refs[:count]
        return out

    x_all, u_one_all, qkv_all, attn_all, hidden_all, u_two_all, z_all, act_all = take(8)
    saved = (x_all, hidden_all, z_all, qkv_all)
    weights = take(4)
    gain_one, gain_two, dx_top = take(3)
    g_ref, gain_out, grad_x, dqkv_hbm, dh_hbm, dz_hbm, dx_mid = take(7)
    dx_hbm = [dx_top] + [dx_mid.at[which] for which in range(n_layers - 1)]
    gs, *vm = take(15)
    load, store = take(2)
    stride = WIDTH // (16 * SUB) // 3
    prologue, piece = backward_pieces(n_layers, stride, saved, weights, gain_one, gain_two, (dqkv_hbm, dh_hbm, dz_hbm), dx_hbm, grad_x, gs, vm, load, store)
    f_refs = []
    for low in range(n_layers):
        u_one, attn_out, u_two, act_lo = (ref.at[n_layers - 1 - low] for ref in (u_one_all, attn_all, u_two_all, act_all))
        f_refs += [u_one, dqkv_hbm.at[low], attn_out, dh_hbm.at[low], u_two, dz_hbm.at[low], act_lo, dx_hbm[low]]
    reduce_body(n_tile, n_dev, prologue, piece, n_layers * PIECES * stride + 2, f_refs, g_ref, gain_out, gs, *refs)


def reduce_body(n_tile, n_dev, prologue, piece, gain_start, f_refs, g_ref, gain_out, gs, gr, gz, gs_s, gs_r, gz_s, gz_r, fa, fb, part, ra, acc, rzb, rza, rb, fin,
                fl_a, fl_b, fs_a, fs_b, fr_a, fr_b,
                ra_s, ra_r, z_s, zb_r, za_r, b_s, b_r, bag_s, bag_r, loc, bc_r, up_s, dn_s, aag_s, aag_r, p1_s, p1_r, p2_s, p2_r):
    toks = f_refs[0].shape[0]
    half = WIDTH // 2
    n_slot = fa.shape[0]
    tiles = [tile for lo in range(0, len(f_refs), 8) for tile in layer_tiles(f_refs[lo:lo + 8])][:n_tile]
    per_tile = half // (8 * SUB)
    n_unit = n_tile * per_tile
    me = lax.axis_index('data')
    core, my_x, my_y, my_z = me % 2, (me // 2) % 2, (me // 4) % 2, me // 8
    top_z = n_dev // 8 - 1
    x_dev, y_dev, pair_dev = me + 2 - 4 * my_x, me + 4 - 8 * my_y, me + 1 - 2 * core
    up_dev, dn_dev = me + 8, me - 8

    barrier = pltpu.get_barrier_semaphore()
    for dev in (x_dev, y_dev, pair_dev):
        pl.semaphore_signal(barrier, inc=1, device_id=(dev,), device_id_type=MESH_ID)

    z_devs = [me + 8 * ((my_z + dist) % (top_z + 1) - my_z) for dist in range(1, top_z + 1)]
    for dev in z_devs:
        pl.semaphore_signal(barrier, inc=1, device_id=(dev,), device_id_type=MESH_ID)
    pl.semaphore_wait(barrier, 3 + top_z)

    def remote(src, dst, send_sem, recv_sem, dev):
        return pltpu.make_async_remote_copy(src_ref=src, dst_ref=dst, send_sem=send_sem, recv_sem=recv_sem, device_id=(dev,), device_id_type=MESH_ID)

    def factor_copies(slot, source):
        lhs, left, rhs, right = source
        mine = pl.ds(pl.multiple_of(left + core * half, 128), half)
        other = pl.ds(pl.multiple_of(left + (1 - core) * half, 128), half)
        lo, hi = pl.ds(0, toks), pl.ds(toks, toks)
        cols = pl.ds(right, WIDTH)
        return (
            pltpu.make_async_copy(lhs.at[:, mine], fa.at[slot, lo], fl_a.at[slot]),
            pltpu.make_async_copy(rhs.at[:, cols], fb.at[slot, lo], fl_b.at[slot]),
            remote(lhs.at[:, other], fa.at[slot, hi], fs_a.at[slot], fr_a.at[slot], pair_dev),
            remote(rhs.at[:, cols], fb.at[slot, hi], fs_b.at[slot], fr_b.at[slot], pair_dev),
        )

    for tile in range(2):
        for copy in factor_copies(tile, tiles[tile]):
            copy.start()

    def stream_stages(s):
        my_a, my_b = (my_x, my_y) if s == 0 else (my_y, my_x)
        a_dev, b_dev = (x_dev, y_dev) if s == 0 else (y_dev, x_dev)

        def root_of(u):
            return (u + 2 * s) % (top_z + 1)

        def part_rows(u, side):
            return pl.ds(pl.multiple_of((u % per_tile) * (8 * SUB) + s * (4 * SUB) + side * (2 * SUB), 8), 2 * SUB)

        def part_at(u, side):
            return part.at[(u // per_tile) % 2, part_rows(u, side)]

        def out_at(u, which, side, b_side=None):
            base = (u // per_tile) * WIDTH + which * half + (u % per_tile) * (8 * SUB) + s * (4 * SUB) + side * (2 * SUB)
            if b_side is None:
                return g_ref.at[pl.ds(pl.multiple_of(base, 8), 2 * SUB)]
            return g_ref.at[pl.ds(pl.multiple_of(base + b_side * SUB, 8), SUB)]

        def a_copy(u):
            k = u % RING
            return remote(part_at(u, 1 - my_a), ra.at[s, k], ra_s.at[s, k], ra_r.at[s, k], a_dev)

        def up_copy(u):
            k = u % RING
            return remote(acc.at[s, k], rzb.at[s, k], z_s.at[s, k], zb_r.at[s, k], up_dev)

        def dn_copy(u):
            k = u % RING
            return remote(acc.at[s, k], rza.at[s, k], z_s.at[s, k], za_r.at[s, k], dn_dev)

        def b_rows(side):
            return pl.ds(pl.multiple_of(side * SUB, 8), SUB)

        def b_copy(u):
            k = u % RING
            return remote(acc.at[s, k, b_rows(1 - my_b)], rb.at[s, k], b_s.at[s, k], b_r.at[s, k], b_dev)

        def bag_copy(u, b_side):
            k = u % RING
            return remote(fin.at[s, k], out_at(u, core, my_a, b_side), bag_s.at[s, k], bag_r.at[s, k], b_dev)

        def loc_copy(u):
            k = u % RING
            return pltpu.make_async_copy(fin.at[s, k], out_at(u, core, my_a, my_b), loc.at[s, k])

        def cast_up(u):
            k = u % RING
            rows = out_at(u, core, my_a)
            return remote(rows, rows, up_s.at[s, k], bc_r.at[s, k], up_dev)

        def cast_dn(u):
            k = u % RING
            rows = out_at(u, core, my_a)
            return remote(rows, rows, dn_s.at[s, k], bc_r.at[s, k], dn_dev)

        def aag_copy(u, side):
            k = u % RING
            rows = out_at(u, core, side)
            return remote(rows, rows, aag_s.at[s, k], aag_r.at[s, k], a_dev)

        def p1_copy(u, which):
            k = u % RING
            rows = out_at(u, which, my_a)
            return remote(rows, rows, p1_s.at[s, k], p1_r.at[s, k], pair_dev)

        def p2_copy(u, which):
            k = u % RING
            rows = out_at(u, which, 1 - my_a)
            return remote(rows, rows, p2_s.at[s, k], p2_r.at[s, k], pair_dev)

        def z_send(u, root):
            @pl.when(my_z < root)
            def _():
                up_copy(u).start()

            @pl.when(my_z > root)
            def _():
                dn_copy(u).start()

        def take_below(u):
            k = u % RING
            up_copy(u).wait_recv()
            acc[s, k] = acc[s, k] + rzb[s, k]

        def take_above(u):
            k = u % RING
            dn_copy(u).wait_recv()
            acc[s, k] = acc[s, k] + rza[s, k]

        def stage_first(u):
            a_copy(u).start()

        def stage_pair(u):
            k = u % RING
            root = root_of(u)
            a_copy(u).wait_recv()
            acc[s, k] = part[(u // per_tile) % 2, part_rows(u, my_a)] + ra[s, k]
            a_copy(u).wait_send()

            @pl.when((my_z == 0) | (my_z == top_z))
            def _():
                z_send(u, root)

        def stage_line(level, u):
            root = root_of(u)

            @pl.when((my_z < root) & (my_z == level))
            def _():
                take_below(u)
                up_copy(u).start()

            @pl.when((my_z > root) & (top_z - my_z == level))
            def _():
                take_above(u)
                dn_copy(u).start()

        def stage_root(u):
            @pl.when(my_z == root_of(u))
            def _():
                @pl.when(my_z > 0)
                def _():
                    take_below(u)

                @pl.when(my_z < top_z)
                def _():
                    take_above(u)

                b_copy(u).start()

        def stage_final(u):
            k = u % RING

            @pl.when(my_z == root_of(u))
            def _():
                b_copy(u).wait_recv()
                fin[s, k] = (acc[s, k, b_rows(my_b)] + rb[s, k]) * (1.0 / n_dev)
                bag_copy(u, my_b).start()
                loc_copy(u).start()
                b_copy(u).wait_send()

        def send_on(u, root):
            @pl.when((my_z >= root) & (my_z < top_z))
            def _():
                cast_up(u).start()

            @pl.when((my_z <= root) & (my_z > 0))
            def _():
                cast_dn(u).start()

            aag_copy(u, my_a).start()
            p1_copy(u, core).start()

        def stage_cast(dist, u):
            root = root_of(u)
            if dist == 0:
                @pl.when(my_z == root)
                def _():
                    loc_copy(u).wait()
                    bag_copy(u, my_b).wait_send()
                    bag_copy(u, 1 - my_b).wait_recv()
                    send_on(u, root)
            else:
                @pl.when((my_z == root + dist) | (my_z == root - dist))
                def _():
                    cast_up(u).wait_recv()
                    up_copy(u).wait_send()
                    send_on(u, root)

        def stage_swap(u):
            aag_copy(u, 1 - my_a).wait_recv()
            p2_copy(u, core).start()

        def stage_done(u):
            root = root_of(u)
            p1_copy(u, 1 - core).wait_recv()
            p2_copy(u, 1 - core).wait_recv()

            @pl.when((my_z >= root) & (my_z < top_z))
            def _():
                cast_up(u).wait_send()

            @pl.when((my_z <= root) & (my_z > 0))
            def _():
                cast_dn(u).wait_send()

            aag_copy(u, my_a).wait_send()
            p1_copy(u, core).wait_send()
            p2_copy(u, core).wait_send()

        stages = [stage_first, stage_pair]
        stages += [functools.partial(stage_line, level) for level in range(1, top_z)]
        stages += [stage_root, stage_final]
        stages += [functools.partial(stage_cast, dist) for dist in range(top_z + 1)]
        stages += [stage_swap, stage_done]
        return stages

    gain_devs = (pair_dev, x_dev, y_dev)

    def gain_copy(hop):
        return remote(gs.at[hop], gr.at[hop], gs_s.at[hop], gs_r.at[hop], gain_devs[hop])

    def gain_line(dist, slot):
        return remote(gs.at[3], gz.at[slot], gz_s.at[dist], gz_r.at[slot], z_devs[dist])

    def gain_steps(t):
        @pl.when(t == gain_start)
        def _():
            gain_copy(0).start()

        for hop in range(1, 4):
            @pl.when(t == gain_start + 4 * hop)
            def _():
                gain_copy(hop - 1).wait()
                gs[hop] = gs[hop - 1] + gr[hop - 1]
                if hop < 3:
                    gain_copy(hop).start()
                else:
                    gz[my_z] = gs[hop]
                    for dist in range(top_z):
                        gain_line(dist, my_z).start()

        @pl.when(t == gain_start + 16)
        def _():
            for dist in range(top_z):
                gain_line(dist, my_z).wait_send()
                gain_line(dist, (my_z + dist + 1) % (top_z + 1)).wait_recv()
            total = gz[0]
            for slot in range(1, top_z + 1):
                total = total + gz[slot]
            gain_out[...] = total * (1.0 / n_dev)

    streams = [stream_stages(0), stream_stages(1)]
    n_stage = len(streams[0])

    def step(t, carry):
        tile = t // per_tile
        gain_steps(t)

        for stage_idx in reversed(range(1, n_stage)):
            u = t - HOP * stage_idx

            @pl.when((u >= 0) & (u < n_unit))
            def _():
                for stages in streams:
                    stages[stage_idx](u)

        @pl.when((t < n_unit) & (t % per_tile == 0))
        def _():
            slot = tile % n_slot
            for copy in factor_copies(slot, tiles[0]):
                copy.wait()
            for lo in range(0, half, 128):
                part[tile % 2, lo:lo + 128, :] = lax.dot_general(
                    fa[slot, :, lo:lo + 128], fb[slot], (((0,), (0,)), ((), ())), preferred_element_type=jnp.float32)

            for later in range(2, n_tile):
                @pl.when(tile + 2 == later)
                def _():
                    for copy in factor_copies(later % n_slot, tiles[later]):
                        copy.start()

        @pl.when(t < n_unit)
        def _():
            for stages in streams:
                stages[0](t)

        piece(t)
        return carry

    gs[0] = jnp.zeros(gs.shape[1:], jnp.float32)
    prologue()
    lax.fori_loop(0, n_unit + HOP * (n_stage - 1), step, 0)


def reduce_tiles(saved, weights, gain_one, gain_two, dx_top, n_tile, n_dev):
    n_layers = n_low = gain_one.shape[0]
    gains = jax.ShapeDtypeStruct((-(-2 * n_layers // 8) * 8, WIDTH), jnp.float32)
    toks = dx_top.shape[0]
    half = WIDTH // 2
    f32, bf16 = jnp.float32, jnp.bfloat16
    dma = pltpu.SemaphoreType.DMA
    slots = pltpu.VMEM((2, RING, 2 * SUB, WIDTH), f32)
    flops = n_tile * 2 * half * 2 * toks * WIDTH
    anyspace, vmem = pl.BlockSpec(memory_space=pl.ANY), pl.BlockSpec(memory_space=pltpu.VMEM)
    operands = list(saved) + list(weights)
    outs = [(((n_tile * WIDTH, WIDTH), f32), anyspace), ((gains.shape, f32), vmem), (((toks, WIDTH), bf16), anyspace),
            (((n_low, toks, 3 * WIDTH), bf16), anyspace), (((n_low, toks, WIDTH), bf16), anyspace), (((n_low, toks, 4 * WIDTH), bf16), anyspace),
            (((n_layers - 1, toks, WIDTH), bf16), anyspace)]
    vm_shapes = [(2, WIDTH, WIDTH), (2, WIDTH, WIDTH), (2, toks, WIDTH), (toks, WIDTH), (WIDTH, WIDTH), (toks, 3 * WIDTH), (WIDTH, 3 * WIDTH), (toks, WIDTH),
                 (toks, 4 * WIDTH), (toks, WIDTH), (toks, 3 * WIDTH), (toks, WIDTH), (toks, WIDTH)]
    return pl.pallas_call(
        functools.partial(reduce_kernel, n_layers, n_tile, n_dev),
        out_shape=tuple(jax.ShapeDtypeStruct(*shape) for shape, _ in outs),
        in_specs=[anyspace] * len(operands) + [vmem, vmem, anyspace],
        out_specs=tuple(spec for _, spec in outs),
        scratch_shapes=[pltpu.VMEM((4,) + gains.shape, f32)] + [pltpu.VMEM(shape, bf16) for shape in vm_shapes] + [
            pltpu.VMEM((toks, WIDTH), f32), dma((12,)), dma((7,)),
            pltpu.VMEM((3,) + gains.shape, f32),
            pltpu.VMEM((n_dev // 8,) + gains.shape, f32),
            dma((3,)), dma((3,)), dma((n_dev // 8 - 1,)), dma((n_dev // 8,)),
            pltpu.VMEM((4, 2 * toks, half), bf16),
            pltpu.VMEM((4, 2 * toks, WIDTH), bf16),
            pltpu.VMEM((2, half, WIDTH), f32),
            slots, slots, slots, slots,
            pltpu.VMEM((2, RING, SUB, WIDTH), f32),
            pltpu.VMEM((2, RING, SUB, WIDTH), f32),
        ] + [dma((4,))] * 6 + [dma((2, RING))] * 19,
        compiler_params=pltpu.CompilerParams(collective_id=0, has_side_effects=True, vmem_limit_bytes=62 * 1024 * 1024),
        cost_estimate=pl.CostEstimate(flops=flops, bytes_accessed=n_tile * WIDTH * WIDTH * 8, transcendentals=0),
        name='reduce_tiles',
    )(*operands, gain_one, gain_two, dx_top)


def spread_kernel(n_layers, src_ref, qkv_ref, out_ref, up_ref, down_ref, buf, read_sem, write_sem):
    moves = []
    for layer in range(n_layers):
        for j in range(TILES):
            if j < 4:
                dst = down_ref.at[layer, pl.ds(j * WIDTH, WIDTH)]
            elif j < 8:
                dst = up_ref.at[layer, :, pl.ds((j - 4) * WIDTH, WIDTH)]
            elif j < 9:
                dst = out_ref.at[layer]
            else:
                dst = qkv_ref.at[layer, :, pl.ds((j - 9) * WIDTH, WIDTH)]
            slot = len(moves) % SPREAD
            moves.append((pltpu.make_async_copy(src_ref.at[pl.ds(((n_layers - 1 - layer) * TILES + j) * WIDTH, WIDTH)], buf.at[slot], read_sem.at[slot]),
                          pltpu.make_async_copy(buf.at[slot], dst, write_sem.at[slot])))
    ahead = SPREAD // 2
    for read, _ in moves[:ahead]:
        read.start()
    for idx, (read, write) in enumerate(moves):
        if idx >= ahead:
            moves[idx - ahead][1].wait()
        if idx + ahead < len(moves):
            moves[idx + ahead][0].start()
        read.wait()
        write.start()
    for _, write in moves[-ahead:]:
        write.wait()


def spread_tiles(tiles, n_layers):
    f32 = jnp.float32
    anyspace = pl.BlockSpec(memory_space=pl.ANY)
    shapes = ((WIDTH, 3 * WIDTH), (WIDTH, WIDTH), (WIDTH, 4 * WIDTH), (4 * WIDTH, WIDTH))
    return pl.pallas_call(
        functools.partial(spread_kernel, n_layers),
        out_shape=tuple(jax.ShapeDtypeStruct((n_layers,) + shape, f32) for shape in shapes),
        in_specs=[anyspace],
        out_specs=(anyspace,) * 4,
        scratch_shapes=[pltpu.VMEM((SPREAD, WIDTH, WIDTH), f32), pltpu.SemaphoreType.DMA((SPREAD,)), pltpu.SemaphoreType.DMA((SPREAD,))],
        compiler_params=pltpu.CompilerParams(vmem_limit_bytes=32 * 1024 * 1024),
        name='spread_tiles',
    )(tiles)


def solution(mesh):
    n_dev = mesh.shape['data']

    def local_step(x_loc, grad_y_loc, gain_one, gain_two, w_qkv, w_out, w_up, w_down):
        n_layers = w_qkv.shape[0]
        weights = (w_qkv, w_out, w_up, w_down)
        saved = forward(x_loc[0], gain_one, gain_two, weights)
        tiles, gain_sum, grad_x = reduce_tiles(saved, weights, gain_one, gain_two, grad_y_loc[0], n_layers * TILES, n_dev)[:3]
        return (grad_x[None], gain_sum[:n_layers], gain_sum[n_layers:2 * n_layers]) + tuple(spread_tiles(tiles, n_layers))

    batch_spec = P('data')
    full_spec = P()
    return jax.shard_map(local_step, mesh=mesh, in_specs=(batch_spec, batch_spec) + (full_spec,) * 6, out_specs=(batch_spec,) + (full_spec,) * 6, check_vma=False)
```

```python
import functools
import math

import jax
import jax.numpy as jnp
from jax import lax
from jax.experimental import pallas as pl
from jax.experimental.pallas import tpu as pltpu
from jax.sharding import PartitionSpec as P

NORM_EPS = 1e-6
HEAD_DIM = 64
WIDTH = 768
TILES = 12
SUB = 8
RING = 16
SPREAD = 8
PIECES = 12
HOP = 2
MESH_ID = pl.DeviceIdType.MESH


def rms_gain(rows_f, gain_vec):
    return rows_f * lax.rsqrt(jnp.mean(rows_f * rows_f, axis=-1, keepdims=True) + NORM_EPS) * gain_vec


def gelu_tanh(pre_act):
    return jax.nn.gelu(pre_act, approximate=True)


def dot_nt(lhs, rhs):
    return lax.dot_general(lhs, rhs, (((1,), (1,)), ((), ())), preferred_element_type=jnp.float32)


def dot_tn(lhs, rhs):
    return lax.dot_general(lhs, rhs, (((0,), (0,)), ((), ())), preferred_element_type=jnp.float32)


def head_probs(q_part, k_pair):
    scores = dot_nt(q_part, k_pair) * HEAD_DIM ** -0.5
    rows = lax.broadcasted_iota(jnp.int32, scores.shape, 0)
    cols = lax.broadcasted_iota(jnp.int32, scores.shape, 1)
    scores = jnp.where(rows >= cols, scores, -1e30)
    weights = jnp.exp(scores - jnp.max(scores, axis=-1, keepdims=True))
    return weights * (1.0 / jnp.sum(weights, axis=-1, keepdims=True))


def pair_masks(shape):
    first = lax.broadcasted_iota(jnp.int32, shape, 1) < HEAD_DIM
    return first, [jnp.where(first, 1.0, 0.0).astype(jnp.bfloat16), jnp.where(first, 0.0, 1.0).astype(jnp.bfloat16)]


def pair_grads(q_pair, k_pair, v_pair, do_pair):
    first, masks = pair_masks(q_pair.shape)
    grads = []
    for mask in masks:
        prob = head_probs(q_pair * mask, k_pair)
        grad_prob = dot_nt(do_pair * mask, v_pair)
        grad_score = (prob * (grad_prob - jnp.sum(prob * grad_prob, axis=-1, keepdims=True)) * HEAD_DIM ** -0.5).astype(jnp.bfloat16)
        grads.append((
            jnp.dot(grad_score, k_pair, preferred_element_type=jnp.float32),
            dot_tn(grad_score, q_pair),
            dot_tn(prob.astype(jnp.bfloat16), do_pair),
        ))
    return [jnp.where(first, grads[0][idx], grads[1][idx]).astype(jnp.bfloat16) for idx in range(3)]


def causal_rows(q_part, k_pair, v_pair, lo, count):
    keys = lo + count
    scores = dot_nt(q_part[lo:keys], k_pair[:keys]) * HEAD_DIM ** -0.5
    rows = lax.broadcasted_iota(jnp.int32, scores.shape, 0) + lo
    cols = lax.broadcasted_iota(jnp.int32, scores.shape, 1)
    scores = jnp.where(rows >= cols, scores, -1e30)
    weights = jnp.exp(scores - jnp.max(scores, axis=-1, keepdims=True))
    probs = (weights * (1.0 / jnp.sum(weights, axis=-1, keepdims=True))).astype(jnp.bfloat16)
    return jnp.dot(probs, v_pair[:keys], preferred_element_type=jnp.float32)


def forward_kernel(n_layers, x_ref, gain_one, gain_two, w_qkv, w_out, w_up, w_down,
                   x_all, u_one_all, qkv_all, attn_all, hidden_all, u_two_all, z_all, act_all,
                   wq, wo, w1, w2, x_v, u_one, qkv, attn, hidden, u_two, z_v, act, acc, load, store):
    f32, bf16 = jnp.float32, jnp.bfloat16
    toks = x_ref.shape[0]

    def loads(layer):
        slot = layer % 2
        return [pltpu.make_async_copy(src.at[layer], dst.at[slot], load.at[slot, idx])
                for idx, (src, dst) in enumerate(((w_qkv, wq), (w_out, wo), (w_up, w1), (w_down, w2)))]

    def saves(layer):
        pairs = ((x_v, x_all), (u_one, u_one_all), (qkv, qkv_all), (attn, attn_all), (hidden, hidden_all), (u_two, u_two_all), (z_v, z_all), (act, act_all))
        return [pltpu.make_async_copy(src, dst.at[layer], store.at[idx]) for idx, (src, dst) in enumerate(pairs)]

    for copy in loads(jnp.int32(0))[:2]:
        copy.start()
    x_v[...] = x_ref[...]

    def layer_step(layer, carry):
        slot = layer % 2
        weights, outs = loads(layer), saves(layer)

        def reuse(idx):
            @pl.when(layer > 0)
            def _():
                outs[idx].wait()

        outs[0].start()
        reuse(1)
        u_one[...] = rms_gain(x_v[...].astype(f32), gain_one[pl.ds(layer, 1), :]).astype(bf16)
        outs[1].start()
        weights[0].wait()

        @pl.when(layer == 0)
        def _():
            weights[2].start()
            weights[3].start()

        reuse(2)
        for j in range(3):
            cols = slice(j * WIDTH, (j + 1) * WIDTH)
            qkv[:, cols] = jnp.dot(u_one[...], wq[slot, :, cols], preferred_element_type=f32).astype(bf16)
        outs[2].start()
        reuse(3)

        @pl.when(layer + 1 < n_layers)
        def _():
            for copy in loads(layer + 1):
                copy.start()


        def pair_step(pair, inner):
            def pair_cols(part_idx):
                return pl.ds(pl.multiple_of(part_idx * WIDTH + pair * 2 * HEAD_DIM, 2 * HEAD_DIM), 2 * HEAD_DIM)

            q_pair, k_pair, v_pair = (qkv[:, pair_cols(part_idx)] for part_idx in range(3))
            first, masks = pair_masks(q_pair.shape)
            heads = [q_pair * mask for mask in masks]
            for lo in range(0, toks, 128):
                out = [causal_rows(head, k_pair, v_pair, lo, 128) for head in heads]
                attn[lo:lo + 128, pair_cols(0)] = jnp.where(first[:128], out[0], out[1]).astype(bf16)
            return inner

        lax.fori_loop(0, WIDTH // (2 * HEAD_DIM), pair_step, 0)
        outs[3].start()
        weights[1].wait()
        mixed = jnp.dot(attn[...], wo[slot], preferred_element_type=f32).astype(bf16)
        reuse(4)
        hidden[...] = (x_v[...].astype(f32) + mixed.astype(f32)).astype(bf16)
        outs[4].start()
        reuse(5)
        u_two[...] = rms_gain(hidden[...].astype(f32), gain_two[pl.ds(layer, 1), :]).astype(bf16)
        outs[5].start()
        weights[2].wait()
        weights[3].wait()
        reuse(6)
        reuse(7)
        for j in range(4):
            cols = slice(j * WIDTH, (j + 1) * WIDTH)
            pre = jnp.dot(u_two[...], w1[slot, :, cols], preferred_element_type=f32).astype(bf16)
            z_v[:, cols] = pre
            act[:, cols] = gelu_tanh(pre.astype(f32)).astype(bf16)

            @pl.when(layer + 1 < n_layers)
            def _():
                term = jnp.dot(act[:, cols], w2[slot, cols], preferred_element_type=f32)
                acc[...] = term if j == 0 else acc[...] + term
        outs[6].start()
        outs[7].start()
        outs[0].wait()

        @pl.when(layer + 1 < n_layers)
        def _():
            x_v[...] = (hidden[...].astype(f32) + acc[...].astype(bf16).astype(f32)).astype(bf16)

        return carry

    lax.fori_loop(0, n_layers, layer_step, 0)
    for copy in saves(n_layers - 1)[1:]:
        copy.wait()


def forward(x_loc, gain_one, gain_two, weights):
    n_layers, toks = gain_one.shape[0], x_loc.shape[0]
    f32, bf16 = jnp.float32, jnp.bfloat16
    anyspace, vmem = pl.BlockSpec(memory_space=pl.ANY), pl.BlockSpec(memory_space=pltpu.VMEM)
    widths = (WIDTH, WIDTH, 3 * WIDTH, WIDTH, WIDTH, WIDTH, 4 * WIDTH, 4 * WIDTH)
    return pl.pallas_call(
        functools.partial(forward_kernel, n_layers),
        out_shape=tuple(jax.ShapeDtypeStruct((n_layers, toks, width), bf16) for width in widths),
        in_specs=[vmem, vmem, vmem] + [anyspace] * 4,
        out_specs=(anyspace,) * 8,
        scratch_shapes=[pltpu.VMEM((2,) + weight.shape[1:], bf16) for weight in weights] + [pltpu.VMEM((toks, width), bf16) for width in widths] + [
            pltpu.VMEM((toks, WIDTH), f32), pltpu.SemaphoreType.DMA((2, 4)), pltpu.SemaphoreType.DMA((8,))],
        compiler_params=pltpu.CompilerParams(vmem_limit_bytes=58 * 1024 * 1024),
        name='forward',
    )(x_loc, gain_one, gain_two, *weights)


def layer_tiles(factors):
    u_one, grad_qkv, attn_out, grad_hidden, u_two, grad_pre, act_lo, grad_blk = factors
    tiles = []
    for lhs, rhs in ((act_lo, grad_blk), (u_two, grad_pre), (attn_out, grad_hidden), (u_one, grad_qkv)):
        tiles += [(lhs, left, rhs, right) for left in range(0, lhs.shape[1], WIDTH) for right in range(0, rhs.shape[1], WIDTH)]
    return tiles


def norm_grad(rows, gain, grad_out):
    scale = lax.rsqrt(jnp.mean(rows * rows, axis=-1, keepdims=True) + NORM_EPS)
    grad_gain = jnp.sum(grad_out * rows * scale, axis=0, keepdims=True)
    grad_unit = grad_out * gain
    grad_rows = grad_unit * scale - rows * (scale * scale * scale) * jnp.mean(rows * grad_unit, axis=-1, keepdims=True)
    return grad_rows, grad_gain


def gelu_slope(z):
    const = (2.0 / math.pi) ** 0.5
    curve = jnp.tanh(const * (z + 0.044715 * (z * z * z)))
    return 0.5 * (1.0 + curve) + 0.5 * z * (1.0 - curve * curve) * const * (1.0 + 3.0 * 0.044715 * (z * z))


def backward_pieces(n_layers, stride, saved, weights, gain_one, gain_two, grads_hbm, dx_hbm, grad_x, gs, vm, load, store):
    w_qkv, w_out, w_up, w_down = weights
    dqkv_hbm, dh_hbm, dz_hbm = grads_hbm
    w2, w1, zb, hb, wo, qkvb, wq, xb, dz, dh, dqkv, dy, do, acc = vm
    n_low = n_layers

    def cols(j):
        return pl.ds(pl.multiple_of(j * WIDTH, WIDTH), WIDTH)

    def weight_loads(low, j):
        layer, slot = n_layers - 1 - low, j % 2
        return (pltpu.make_async_copy(w_down.at[layer, cols(j)], w2.at[slot], load.at[slot]),
                pltpu.make_async_copy(w_up.at[layer, :, cols(j)], w1.at[slot], load.at[2 + slot]))

    def saved_load(kind, low, src_cols, dst, sem, act):
        layer = n_layers - 1 - low
        src = saved[kind].at[layer] if src_cols is None else saved[kind].at[layer, :, src_cols]
        getattr(pltpu.make_async_copy(src, dst, sem), act)()

    def mlp_loads(low, j, act):
        for copy in weight_loads(low, j):
            getattr(copy, act)()
        saved_load(2, low, cols(j), zb.at[j % 2], load.at[4 + j % 2], act)

    def attn_loads(low, act):
        getattr(pltpu.make_async_copy(w_out.at[n_layers - 1 - low], wo, load.at[6]), act)()
        saved_load(1, low, None, hb, load.at[7], act)

    def last_loads(low, act):
        getattr(pltpu.make_async_copy(w_qkv.at[n_layers - 1 - low], wq, load.at[9]), act)()
        saved_load(0, low, None, xb, load.at[10], act)

    def add_gain(row, value):
        rows = lax.broadcasted_iota(jnp.int32, gs.shape[1:], 0)
        gs[0] = gs[0] + jnp.where(rows == row, value, 0.0)

    def prologue():
        first = pltpu.make_async_copy(dx_hbm[0], dy, load.at[11])
        first.start()
        mlp_loads(jnp.int32(0), jnp.int32(0), 'start')
        first.wait()

    def dz_out(low, j):
        return pltpu.make_async_copy(dz.at[:, cols(j)], dz_hbm.at[low, :, cols(j)], store.at[j])

    def piece(t):
        slow = t - 1 - PIECES * stride
        count = jnp.where(slow < 0, (t - 1) // stride, PIECES + slow // (2 * stride))
        due = jnp.where(slow < 0, (t - 1) % stride, slow % (2 * stride)) == 0
        low, p = count // PIECES, count % PIECES
        layer = n_layers - 1 - low
        active = (t >= 1) & due & (count < n_low * PIECES)

        @pl.when(active & (p < 4))
        def _():
            mlp_loads(low, p, 'wait')

            @pl.when(p < 3)
            def _():
                mlp_loads(low, p + 1, 'start')

            @pl.when(p == 3)
            def _():
                attn_loads(low, 'start')
                saved_load(3, low, None, qkvb, load.at[8], 'start')

            slot = p % 2
            grad_act = dot_nt(dy[...], w2[slot]).astype(jnp.bfloat16).astype(jnp.float32)
            grad_pre = (gelu_slope(zb[slot].astype(jnp.float32)) * grad_act).astype(jnp.bfloat16)
            dz[:, cols(p)] = grad_pre
            term = dot_nt(grad_pre, w1[slot])

            @pl.when(p == 0)
            def _():
                acc[...] = term

            @pl.when(p > 0)
            def _():
                acc[...] = acc[...] + term

            dz_out(low, p).start()

        @pl.when(active & (p == 4))
        def _():
            attn_loads(low, 'wait')
            last_loads(low, 'start')
            grad_out = acc[...].astype(jnp.bfloat16).astype(jnp.float32)
            gain = gain_two[pl.ds(layer, 1), :]
            grad_rows, grad_gain = norm_grad(hb[...].astype(jnp.float32), gain, grad_out)
            dh[...] = (dy[...].astype(jnp.float32) + grad_rows).astype(jnp.bfloat16)
            add_gain(n_layers + layer, grad_gain)
            do[...] = dot_nt(dh[...], wo[...]).astype(jnp.bfloat16)
            pltpu.make_async_copy(dh, dh_hbm.at[low], store.at[4]).start()
            saved_load(3, low, None, qkvb, load.at[8], 'wait')
            for j in range(4):
                dz_out(low, j).wait()

        @pl.when(active & (p >= 5) & (p < 11))
        def _():
            def pair_cols(part_idx):
                return pl.ds(pl.multiple_of(part_idx * WIDTH + (p - 5) * 2 * HEAD_DIM, 2 * HEAD_DIM), 2 * HEAD_DIM)

            pair = pair_grads(qkvb[:, pair_cols(0)], qkvb[:, pair_cols(1)], qkvb[:, pair_cols(2)], do[:, pair_cols(0)])
            for part_idx in range(3):
                dqkv[:, pair_cols(part_idx)] = pair[part_idx]

        @pl.when(active & (p == 11))
        def _():
            last_loads(low, 'wait')
            dqkv_out = pltpu.make_async_copy(dqkv, dqkv_hbm.at[low], store.at[5])
            dqkv_out.start()

            @pl.when(low + 1 < n_low)
            def _():
                mlp_loads(low + 1, jnp.int32(0), 'start')

            grad_out = dot_nt(dqkv[...], wq[...]).astype(jnp.bfloat16).astype(jnp.float32)
            gain = gain_one[pl.ds(layer, 1), :]
            grad_rows, grad_gain = norm_grad(xb[...].astype(jnp.float32), gain, grad_out)
            add_gain(layer, grad_gain)
            dy[...] = (dh[...].astype(jnp.float32) + grad_rows).astype(jnp.bfloat16)
            for which in range(n_low):
                dst = grad_x if which == n_low - 1 else dx_hbm[which + 1]

                @pl.when(low == which)
                def _():
                    out = pltpu.make_async_copy(dy, dst, store.at[6])
                    out.start()
                    out.wait()

            pltpu.make_async_copy(dh, dh_hbm.at[low], store.at[4]).wait()
            dqkv_out.wait()

    return prologue, piece


def reduce_kernel(n_layers, n_tile, n_dev, *refs):
    refs = list(refs)

    def take(count):
        out = refs[:count]
        del refs[:count]
        return out

    x_all, u_one_all, qkv_all, attn_all, hidden_all, u_two_all, z_all, act_all = take(8)
    saved = (x_all, hidden_all, z_all, qkv_all)
    weights = take(4)
    gain_one, gain_two, dx_top = take(3)
    g_ref, gain_out, grad_x, dqkv_hbm, dh_hbm, dz_hbm, dx_mid = take(7)
    dx_hbm = [dx_top] + [dx_mid.at[which] for which in range(n_layers - 1)]
    gs, *vm = take(15)
    load, store = take(2)
    stride = WIDTH // (16 * SUB) // 3
    prologue, piece = backward_pieces(n_layers, stride, saved, weights, gain_one, gain_two, (dqkv_hbm, dh_hbm, dz_hbm), dx_hbm, grad_x, gs, vm, load, store)
    f_refs = []
    for low in range(n_layers):
        u_one, attn_out, u_two, act_lo = (ref.at[n_layers - 1 - low] for ref in (u_one_all, attn_all, u_two_all, act_all))
        f_refs += [u_one, dqkv_hbm.at[low], attn_out, dh_hbm.at[low], u_two, dz_hbm.at[low], act_lo, dx_hbm[low]]
    reduce_body(n_tile, n_dev, prologue, piece, (2 * n_layers - 1) * PIECES * stride + 2, f_refs, g_ref, gain_out, gs, *refs)


def reduce_body(n_tile, n_dev, prologue, piece, gain_start, f_refs, g_ref, gain_out, gs, gr, gz, gs_s, gs_r, gz_s, gz_r, fa, fb, part, ra, acc, rzb, rza, rb, fin,
                fl_a, fl_b, fs_a, fs_b, fr_a, fr_b,
                ra_s, ra_r, z_s, zb_r, za_r, b_s, b_r, bag_s, bag_r, loc, bc_r, up_s, dn_s, aag_s, aag_r, p1_s, p1_r, p2_s, p2_r):
    toks = f_refs[0].shape[0]
    half = WIDTH // 2
    n_slot = fa.shape[0]
    tiles = [tile for lo in range(0, len(f_refs), 8) for tile in layer_tiles(f_refs[lo:lo + 8])][:n_tile]
    per_tile = half // (8 * SUB)
    n_unit = n_tile * per_tile
    me = lax.axis_index('data')
    core, my_x, my_y, my_z = me % 2, (me // 2) % 2, (me // 4) % 2, me // 8
    top_z = n_dev // 8 - 1
    x_dev, y_dev, pair_dev = me + 2 - 4 * my_x, me + 4 - 8 * my_y, me + 1 - 2 * core
    up_dev, dn_dev = me + 8, me - 8

    barrier = pltpu.get_barrier_semaphore()
    for dev in (x_dev, y_dev, pair_dev):
        pl.semaphore_signal(barrier, inc=1, device_id=(dev,), device_id_type=MESH_ID)

    z_devs = [me + 8 * ((my_z + dist) % (top_z + 1) - my_z) for dist in range(1, top_z + 1)]
    for dev in z_devs:
        pl.semaphore_signal(barrier, inc=1, device_id=(dev,), device_id_type=MESH_ID)
    pl.semaphore_wait(barrier, 3 + top_z)

    def remote(src, dst, send_sem, recv_sem, dev):
        return pltpu.make_async_remote_copy(src_ref=src, dst_ref=dst, send_sem=send_sem, recv_sem=recv_sem, device_id=(dev,), device_id_type=MESH_ID)

    def factor_copies(slot, source):
        lhs, left, rhs, right = source
        mine = pl.ds(pl.multiple_of(left + core * half, 128), half)
        other = pl.ds(pl.multiple_of(left + (1 - core) * half, 128), half)
        lo, hi = pl.ds(0, toks), pl.ds(toks, toks)
        cols = pl.ds(right, WIDTH)
        return (
            pltpu.make_async_copy(lhs.at[:, mine], fa.at[slot, lo], fl_a.at[slot]),
            pltpu.make_async_copy(rhs.at[:, cols], fb.at[slot, lo], fl_b.at[slot]),
            remote(lhs.at[:, other], fa.at[slot, hi], fs_a.at[slot], fr_a.at[slot], pair_dev),
            remote(rhs.at[:, cols], fb.at[slot, hi], fs_b.at[slot], fr_b.at[slot], pair_dev),
        )

    for tile in range(2):
        for copy in factor_copies(tile, tiles[tile]):
            copy.start()

    def stream_stages(s):
        my_a, my_b = (my_x, my_y) if s == 0 else (my_y, my_x)
        a_dev, b_dev = (x_dev, y_dev) if s == 0 else (y_dev, x_dev)

        def root_of(u):
            return (u + 2 * s) % (top_z + 1)

        def part_rows(u, side):
            return pl.ds(pl.multiple_of((u % per_tile) * (8 * SUB) + s * (4 * SUB) + side * (2 * SUB), 8), 2 * SUB)

        def part_at(u, side):
            return part.at[(u // per_tile) % 2, part_rows(u, side)]

        def out_at(u, which, side, b_side=None):
            base = (u // per_tile) * WIDTH + which * half + (u % per_tile) * (8 * SUB) + s * (4 * SUB) + side * (2 * SUB)
            if b_side is None:
                return g_ref.at[pl.ds(pl.multiple_of(base, 8), 2 * SUB)]
            return g_ref.at[pl.ds(pl.multiple_of(base + b_side * SUB, 8), SUB)]

        def a_copy(u):
            k = u % RING
            return remote(part_at(u, 1 - my_a), ra.at[s, k], ra_s.at[s, k], ra_r.at[s, k], a_dev)

        def up_copy(u):
            k = u % RING
            return remote(acc.at[s, k], rzb.at[s, k], z_s.at[s, k], zb_r.at[s, k], up_dev)

        def dn_copy(u):
            k = u % RING
            return remote(acc.at[s, k], rza.at[s, k], z_s.at[s, k], za_r.at[s, k], dn_dev)

        def b_rows(side):
            return pl.ds(pl.multiple_of(side * SUB, 8), SUB)

        def b_copy(u):
            k = u % RING
            return remote(acc.at[s, k, b_rows(1 - my_b)], rb.at[s, k], b_s.at[s, k], b_r.at[s, k], b_dev)

        def bag_copy(u, b_side):
            k = u % RING
            return remote(fin.at[s, k], out_at(u, core, my_a, b_side), bag_s.at[s, k], bag_r.at[s, k], b_dev)

        def loc_copy(u):
            k = u % RING
            return pltpu.make_async_copy(fin.at[s, k], out_at(u, core, my_a, my_b), loc.at[s, k])

        def cast_up(u):
            k = u % RING
            rows = out_at(u, core, my_a)
            return remote(rows, rows, up_s.at[s, k], bc_r.at[s, k], up_dev)

        def cast_dn(u):
            k = u % RING
            rows = out_at(u, core, my_a)
            return remote(rows, rows, dn_s.at[s, k], bc_r.at[s, k], dn_dev)

        def aag_copy(u, side):
            k = u % RING
            rows = out_at(u, core, side)
            return remote(rows, rows, aag_s.at[s, k], aag_r.at[s, k], a_dev)

        def p1_copy(u, which):
            k = u % RING
            rows = out_at(u, which, my_a)
            return remote(rows, rows, p1_s.at[s, k], p1_r.at[s, k], pair_dev)

        def p2_copy(u, which):
            k = u % RING
            rows = out_at(u, which, 1 - my_a)
            return remote(rows, rows, p2_s.at[s, k], p2_r.at[s, k], pair_dev)

        def z_send(u, root):
            @pl.when(my_z < root)
            def _():
                up_copy(u).start()

            @pl.when(my_z > root)
            def _():
                dn_copy(u).start()

        def take_below(u):
            k = u % RING
            up_copy(u).wait_recv()
            acc[s, k] = acc[s, k] + rzb[s, k]

        def take_above(u):
            k = u % RING
            dn_copy(u).wait_recv()
            acc[s, k] = acc[s, k] + rza[s, k]

        def stage_first(u):
            a_copy(u).start()

        def stage_pair(u):
            k = u % RING
            root = root_of(u)
            a_copy(u).wait_recv()
            acc[s, k] = part[(u // per_tile) % 2, part_rows(u, my_a)] + ra[s, k]
            a_copy(u).wait_send()

            @pl.when((my_z == 0) | (my_z == top_z))
            def _():
                z_send(u, root)

        def stage_line(level, u):
            root = root_of(u)

            @pl.when((my_z < root) & (my_z == level))
            def _():
                take_below(u)
                up_copy(u).start()

            @pl.when((my_z > root) & (top_z - my_z == level))
            def _():
                take_above(u)
                dn_copy(u).start()

        def stage_root(u):
            @pl.when(my_z == root_of(u))
            def _():
                @pl.when(my_z > 0)
                def _():
                    take_below(u)

                @pl.when(my_z < top_z)
                def _():
                    take_above(u)

                b_copy(u).start()

        def stage_final(u):
            k = u % RING

            @pl.when(my_z == root_of(u))
            def _():
                b_copy(u).wait_recv()
                fin[s, k] = (acc[s, k, b_rows(my_b)] + rb[s, k]) * (1.0 / n_dev)
                bag_copy(u, my_b).start()
                loc_copy(u).start()
                b_copy(u).wait_send()

        def send_on(u, root):
            @pl.when((my_z >= root) & (my_z < top_z))
            def _():
                cast_up(u).start()

            @pl.when((my_z <= root) & (my_z > 0))
            def _():
                cast_dn(u).start()

            aag_copy(u, my_a).start()
            p1_copy(u, core).start()

        def stage_cast(dist, u):
            root = root_of(u)
            if dist == 0:
                @pl.when(my_z == root)
                def _():
                    loc_copy(u).wait()
                    bag_copy(u, my_b).wait_send()
                    bag_copy(u, 1 - my_b).wait_recv()
                    send_on(u, root)
            else:
                @pl.when((my_z == root + dist) | (my_z == root - dist))
                def _():
                    cast_up(u).wait_recv()
                    up_copy(u).wait_send()
                    send_on(u, root)

        def stage_swap(u):
            aag_copy(u, 1 - my_a).wait_recv()
            p2_copy(u, core).start()

        def stage_done(u):
            root = root_of(u)
            p1_copy(u, 1 - core).wait_recv()
            p2_copy(u, 1 - core).wait_recv()

            @pl.when((my_z >= root) & (my_z < top_z))
            def _():
                cast_up(u).wait_send()

            @pl.when((my_z <= root) & (my_z > 0))
            def _():
                cast_dn(u).wait_send()

            aag_copy(u, my_a).wait_send()
            p1_copy(u, core).wait_send()
            p2_copy(u, core).wait_send()

        stages = [stage_first, stage_pair]
        stages += [functools.partial(stage_line, level) for level in range(1, top_z)]
        stages += [stage_root, stage_final]
        stages += [functools.partial(stage_cast, dist) for dist in range(top_z + 1)]
        stages += [stage_swap, stage_done]
        return stages

    gain_devs = (pair_dev, x_dev, y_dev)

    def gain_copy(hop):
        return remote(gs.at[hop], gr.at[hop], gs_s.at[hop], gs_r.at[hop], gain_devs[hop])

    def gain_line(dist, slot):
        return remote(gs.at[3], gz.at[slot], gz_s.at[dist], gz_r.at[slot], z_devs[dist])

    def gain_steps(t):
        @pl.when(t == gain_start)
        def _():
            gain_copy(0).start()

        for hop in range(1, 4):
            @pl.when(t == gain_start + 4 * hop)
            def _():
                gain_copy(hop - 1).wait()
                gs[hop] = gs[hop - 1] + gr[hop - 1]
                if hop < 3:
                    gain_copy(hop).start()
                else:
                    gz[my_z] = gs[hop]
                    for dist in range(top_z):
                        gain_line(dist, my_z).start()

        @pl.when(t == gain_start + 16)
        def _():
            for dist in range(top_z):
                gain_line(dist, my_z).wait_send()
                gain_line(dist, (my_z + dist + 1) % (top_z + 1)).wait_recv()
            total = gz[0]
            for slot in range(1, top_z + 1):
                total = total + gz[slot]
            gain_out[...] = total * (1.0 / n_dev)

    streams = [stream_stages(0), stream_stages(1)]
    n_stage = len(streams[0])

    def step(t, carry):
        tile = t // per_tile
        gain_steps(t)

        for stage_idx in reversed(range(1, n_stage)):
            u = t - HOP * stage_idx

            @pl.when((u >= 0) & (u < n_unit))
            def _():
                for stages in streams:
                    stages[stage_idx](u)

        @pl.when((t < n_unit) & (t % per_tile == 0))
        def _():
            slot = tile % n_slot
            for copy in factor_copies(slot, tiles[0]):
                copy.wait()
            for lo in range(0, half, 128):
                part[tile % 2, lo:lo + 128, :] = lax.dot_general(
                    fa[slot, :, lo:lo + 128], fb[slot], (((0,), (0,)), ((), ())), preferred_element_type=jnp.float32)

            for later in range(2, n_tile):
                @pl.when(tile + 2 == later)
                def _():
                    for copy in factor_copies(later % n_slot, tiles[later]):
                        copy.start()

        @pl.when(t < n_unit)
        def _():
            for stages in streams:
                stages[0](t)

        piece(t)
        return carry

    gs[0] = jnp.zeros(gs.shape[1:], jnp.float32)
    prologue()
    lax.fori_loop(0, n_unit + HOP * (n_stage - 1), step, 0)


def reduce_tiles(saved, weights, gain_one, gain_two, dx_top, n_tile, n_dev):
    n_layers = n_low = gain_one.shape[0]
    gains = jax.ShapeDtypeStruct((-(-2 * n_layers // 8) * 8, WIDTH), jnp.float32)
    toks = dx_top.shape[0]
    half = WIDTH // 2
    f32, bf16 = jnp.float32, jnp.bfloat16
    dma = pltpu.SemaphoreType.DMA
    slots = pltpu.VMEM((2, RING, 2 * SUB, WIDTH), f32)
    flops = n_tile * 2 * half * 2 * toks * WIDTH
    anyspace, vmem = pl.BlockSpec(memory_space=pl.ANY), pl.BlockSpec(memory_space=pltpu.VMEM)
    operands = list(saved) + list(weights)
    outs = [(((n_tile * WIDTH, WIDTH), f32), anyspace), ((gains.shape, f32), vmem), (((toks, WIDTH), bf16), anyspace),
            (((n_low, toks, 3 * WIDTH), bf16), anyspace), (((n_low, toks, WIDTH), bf16), anyspace), (((n_low, toks, 4 * WIDTH), bf16), anyspace),
            (((n_layers - 1, toks, WIDTH), bf16), anyspace)]
    vm_shapes = [(2, WIDTH, WIDTH), (2, WIDTH, WIDTH), (2, toks, WIDTH), (toks, WIDTH), (WIDTH, WIDTH), (toks, 3 * WIDTH), (WIDTH, 3 * WIDTH), (toks, WIDTH),
                 (toks, 4 * WIDTH), (toks, WIDTH), (toks, 3 * WIDTH), (toks, WIDTH), (toks, WIDTH)]
    return pl.pallas_call(
        functools.partial(reduce_kernel, n_layers, n_tile, n_dev),
        out_shape=tuple(jax.ShapeDtypeStruct(*shape) for shape, _ in outs),
        in_specs=[anyspace] * len(operands) + [vmem, vmem, anyspace],
        out_specs=tuple(spec for _, spec in outs),
        scratch_shapes=[pltpu.VMEM((4,) + gains.shape, f32)] + [pltpu.VMEM(shape, bf16) for shape in vm_shapes] + [
            pltpu.VMEM((toks, WIDTH), f32), dma((12,)), dma((7,)),
            pltpu.VMEM((3,) + gains.shape, f32),
            pltpu.VMEM((n_dev // 8,) + gains.shape, f32),
            dma((3,)), dma((3,)), dma((n_dev // 8 - 1,)), dma((n_dev // 8,)),
            pltpu.VMEM((4, 2 * toks, half), bf16),
            pltpu.VMEM((4, 2 * toks, WIDTH), bf16),
            pltpu.VMEM((2, half, WIDTH), f32),
            slots, slots, slots, slots,
            pltpu.VMEM((2, RING, SUB, WIDTH), f32),
            pltpu.VMEM((2, RING, SUB, WIDTH), f32),
        ] + [dma((4,))] * 6 + [dma((2, RING))] * 19,
        compiler_params=pltpu.CompilerParams(collective_id=0, has_side_effects=True, vmem_limit_bytes=62 * 1024 * 1024),
        cost_estimate=pl.CostEstimate(flops=flops, bytes_accessed=n_tile * WIDTH * WIDTH * 8, transcendentals=0),
        name='reduce_tiles',
    )(*operands, gain_one, gain_two, dx_top)


def spread_kernel(n_layers, src_ref, qkv_ref, out_ref, up_ref, down_ref, buf, read_sem, write_sem):
    moves = []
    for layer in range(n_layers):
        for j in range(TILES):
            if j < 4:
                dst = down_ref.at[layer, pl.ds(j * WIDTH, WIDTH)]
            elif j < 8:
                dst = up_ref.at[layer, :, pl.ds((j - 4) * WIDTH, WIDTH)]
            elif j < 9:
                dst = out_ref.at[layer]
            else:
                dst = qkv_ref.at[layer, :, pl.ds((j - 9) * WIDTH, WIDTH)]
            slot = len(moves) % SPREAD
            moves.append((pltpu.make_async_copy(src_ref.at[pl.ds(((n_layers - 1 - layer) * TILES + j) * WIDTH, WIDTH)], buf.at[slot], read_sem.at[slot]),
                          pltpu.make_async_copy(buf.at[slot], dst, write_sem.at[slot])))
    ahead = SPREAD // 2
    for read, _ in moves[:ahead]:
        read.start()
    for idx, (read, write) in enumerate(moves):
        if idx >= ahead:
            moves[idx - ahead][1].wait()
        if idx + ahead < len(moves):
            moves[idx + ahead][0].start()
        read.wait()
        write.start()
    for _, write in moves[-ahead:]:
        write.wait()


def spread_tiles(tiles, n_layers):
    f32 = jnp.float32
    anyspace = pl.BlockSpec(memory_space=pl.ANY)
    shapes = ((WIDTH, 3 * WIDTH), (WIDTH, WIDTH), (WIDTH, 4 * WIDTH), (4 * WIDTH, WIDTH))
    return pl.pallas_call(
        functools.partial(spread_kernel, n_layers),
        out_shape=tuple(jax.ShapeDtypeStruct((n_layers,) + shape, f32) for shape in shapes),
        in_specs=[anyspace],
        out_specs=(anyspace,) * 4,
        scratch_shapes=[pltpu.VMEM((SPREAD, WIDTH, WIDTH), f32), pltpu.SemaphoreType.DMA((SPREAD,)), pltpu.SemaphoreType.DMA((SPREAD,))],
        compiler_params=pltpu.CompilerParams(vmem_limit_bytes=32 * 1024 * 1024),
        name='spread_tiles',
    )(tiles)


def solution(mesh):
    n_dev = mesh.shape['data']

    def local_step(x_loc, grad_y_loc, gain_one, gain_two, w_qkv, w_out, w_up, w_down):
        n_layers = w_qkv.shape[0]
        weights = (w_qkv, w_out, w_up, w_down)
        saved = forward(x_loc[0], gain_one, gain_two, weights)
        tiles, gain_sum, grad_x = reduce_tiles(saved, weights, gain_one, gain_two, grad_y_loc[0], n_layers * TILES, n_dev)[:3]
        return (grad_x[None], gain_sum[:n_layers], gain_sum[n_layers:2 * n_layers]) + tuple(spread_tiles(tiles, n_layers))

    batch_spec = P('data')
    full_spec = P()
    return jax.shard_map(local_step, mesh=mesh, in_specs=(batch_spec, batch_spec) + (full_spec,) * 6, out_specs=(batch_spec,) + (full_spec,) * 6, check_vma=False)
```
